256 devices in a mesh: batch: 32 (over z_lo, x, core), seq: 8 (over y, z_hi).
Axes of the slice: x: 4, y: 4, z: 8 (z_hi: 2, z_lo: 4; z = z_hi * 4 + z_lo), core: 2. Of those that a mesh axis runs over, the one named last changes fastest.
Arguments:
- tokens: bfloat16 [32, 4096, 2560], P('batch', 'seq'), may hold values from -6 to 6
- attn_in: bfloat16 [32, 4096, 2560], P('batch', 'seq'), may hold values from -6 to 6
- lengths: int32 [32], P('batch'), may hold values from 1024 to 4096
- norm_gain: float32 [2560], replicated, may hold values from 0.5 to 1.5
- attn_gain: float32 [2560], replicated, may hold values from 0.5 to 1.5
- w_x: bfloat16 [2560, 2560], P(('batch', 'seq')), may hold values from -0.125 to 0.125
- conv_w: float32 [4, 2560], replicated, may hold values from -3 to 3
- w_a: bfloat16 [10, 256, 256], replicated, may hold values from -0.375 to 0.375
- w_i: bfloat16 [10, 256, 256], replicated, may hold values from -0.375 to 0.375
- lru_decay: float32 [2560], replicated, may hold values from 4 to 20
- w_kv: bfloat16 [2560, 512], replicated, may hold values from -0.125 to 0.125
Outputs:
- lru_state: float32 [32, 2560], P('batch', 'seq')
- conv_state: bfloat16 [32, 3, 2560], P('batch', None, 'seq')
- kv_cache: bfloat16 [32, 2048, 512], P('batch', None, 'seq')
The draws below stay inside these ranges and needn't reach their ends.
Inputs may be any that keep to these rules, and one draw needn't show every extreme that they name: `lengths`: positions from a prompt's length on are padding.
All inputs are finite; a program needn't handle non-finite values.
Results may differ from the reference program's by a relative error of at most 0.0051.
Values may be sent and summed in bfloat16 or wider, within the bound.
A program may use at most 128 MiB of HBM per device.

```python
import jax
import jax.numpy as jnp
from jax import lax

D = 2560
H = 10
HD = 256
W = 2048
SEQ = 4096
PROMPTS = 32


def draw_lru_decay(key, part):
    pick_key = jax.random.fold_in(key, 11)
    slow_key = jax.random.fold_in(key, 12)
    fast_key = jax.random.fold_in(key, 13)
    share = 50
    fast_mask = jax.random.randint(pick_key, (D,), 0, 100) < share
    slow_value = jnp.log(8.0 * SEQ / jax.random.uniform(slow_key, (D,), jnp.float32, 0.2, 1.0))
    fast_value = jnp.log(jax.random.uniform(fast_key, (D,), jnp.float32, 120.0, 200.0))
    return jnp.where(fast_mask, fast_value, slow_value).astype(jnp.float32)


def place_ends(array, own_key, smallest, largest):
    index_at = [jax.random.randint(jax.random.fold_in(own_key, axis), (), 0, length) for axis, length in enumerate(array.shape)]
    widest = array.shape.index(max(array.shape))
    beside = index_at[:widest] + [(index_at[widest] + 1) % array.shape[widest]] + index_at[widest + 1:]
    return array.at[tuple(index_at)].set(smallest).at[tuple(beside)].set(largest)


def shard_levels(stream_key, shape, pieces, smallest, largest):
    def one(axis_at, blocks):
        heights = jax.random.uniform(jax.random.fold_in(jax.random.fold_in(stream_key, 6), axis_at), (blocks,), jnp.float32, smallest / len(pieces), largest / len(pieces))
        return jnp.repeat(jnp.exp(heights), shape[axis_at] // blocks).reshape((-1,) + (1,) * (len(shape) - axis_at - 1))

    loudness = one(*pieces[0])
    for cut in pieces[1:]:
        loudness = loudness * one(*cut)
    return loudness


def noise(rng, dims, spread, reach, pieces=(), kind=jnp.bfloat16):
    result = jax.random.normal(rng, dims, jnp.float32) * spread
    if len(pieces) > 0:
        result = shard_levels(rng, dims, pieces, -0.22, 0.18) * result
    return jnp.clip(result, min=-reach, max=reach).astype(kind)


def setup_inputs(seed: int = 0) -> dict:
    key_list = jax.random.split(jax.random.key(seed), 12)
    return {
        "tokens": noise(key_list[0], (PROMPTS, SEQ, D), 1.0, 6.0, ((0, 32), (1, 8))),
        "attn_in": noise(key_list[1], (PROMPTS, SEQ, D), 1.0, 6.0, ((0, 32), (1, 8))),
        "lengths": place_ends(jax.random.randint(key_list[2], (PROMPTS,), SEQ // 4, SEQ + 1), jax.random.fold_in(key_list[2], 1), SEQ // 4, SEQ).astype(jnp.int32),
        "norm_gain": jnp.clip(1.0 + 0.1 * jax.random.normal(key_list[3], (D,), jnp.float32), 0.5, 1.5),
        "attn_gain": jnp.clip(1.0 + 0.1 * jax.random.normal(key_list[4], (D,), jnp.float32), 0.5, 1.5),
        "w_x": noise(key_list[5], (D, D), D ** -0.5, 0.125, ((0, 256),)),
        "conv_w": noise(key_list[6], (4, D), 0.5, 3.0, (), jnp.float32),
        "w_a": noise(key_list[7], (H, HD, HD), HD ** -0.5, 0.375),
        "w_i": noise(key_list[8], (H, HD, HD), HD ** -0.5, 0.375),
        "lru_decay": draw_lru_decay(jax.random.fold_in(key_list[11], 71), 0),
        "w_kv": noise(key_list[10], (D, 2 * HD), D ** -0.5, 0.125),
    }


def rms_norm(values, gain_vec):
    widened = values.astype(jnp.float32)
    inverse = lax.rsqrt(lax.optimization_barrier(jnp.mean(widened * widened, axis=-1, keepdims=True)) + 1e-06)
    return (widened * inverse * gain_vec).astype(jnp.bfloat16)

def rotate_keys(key_rows, positions):
    quarter = key_rows.shape[-1] // 4
    spacing = jnp.exp(-jnp.log(10000.0) * jnp.arange(quarter, dtype=jnp.float32) / quarter)
    angles = positions.astype(jnp.float32)[:, None] * spacing[None, :]
    cosine_rows = jnp.cos(angles)
    sine_rows = jnp.sin(angles)
    first_part = key_rows[:, :quarter]
    second_part = key_rows[:, quarter:2 * quarter]
    return jnp.concatenate([first_part * cosine_rows - second_part * sine_rows, second_part * cosine_rows + first_part * sine_rows, key_rows[:, 2 * quarter:]], axis=1)

def one_prompt(norm_gain, attn_gain, w_x, conv_w, w_a, w_i, lru_decay, w_kv, tokens, attn_in, length):
    seq_len = tokens.shape[0]
    normed = rms_norm(tokens, norm_gain)
    x_proj = jnp.dot(normed, w_x, preferred_element_type=jnp.float32).astype(jnp.bfloat16)
    padded = jnp.concatenate([jnp.zeros((3, D), jnp.bfloat16), x_proj], axis=0)
    conv_sum = conv_w[0] * padded[0:seq_len].astype(jnp.float32)
    for offset in range(1, 4):
        conv_sum = conv_sum + conv_w[offset] * padded[offset:offset + seq_len].astype(jnp.float32)
    x_conv = conv_sum.astype(jnp.bfloat16)
    head_rows = x_conv.astype(jnp.float32).reshape(seq_len, H, HD)
    gate_a = jnp.einsum('lhk,hkj->lhj', head_rows, w_a.astype(jnp.float32)).reshape(seq_len, D)
    gate_i = jnp.einsum('lhk,hkj->lhj', head_rows, w_i.astype(jnp.float32)).reshape(seq_len, D)
    positions = jnp.arange(seq_len, dtype=jnp.int32)
    valid_row = (positions < length).astype(jnp.float32)[:, None]
    log_rate = -8.0 * jax.nn.softplus(-lru_decay) * jax.nn.sigmoid(gate_a)
    keep_rate = jnp.exp(log_rate * valid_row)
    push_term = jnp.sqrt(-jnp.expm1(2.0 * log_rate)) * jax.nn.sigmoid(gate_i) * x_conv.astype(jnp.float32) * valid_row

    def advance(carried, step_pair):
        return (step_pair[0] * carried + step_pair[1], None)
    lru_state = lax.scan(advance, jnp.zeros((D,), jnp.float32), (keep_rate, push_term))[0]
    conv_state = lax.dynamic_slice_in_dim(padded, length.astype(jnp.int32), 3, 0)
    attn_normed = rms_norm(attn_in, attn_gain)
    kv_full = jnp.dot(attn_normed, w_kv, preferred_element_type=jnp.float32)
    kv_rows = jnp.concatenate([rotate_keys(kv_full[:, :HD], positions), kv_full[:, HD:]], axis=1).astype(jnp.bfloat16)
    in_window = ((positions >= length - W) & (positions < length)).astype(jnp.float32)[:, None]
    masked = kv_rows.astype(jnp.float32) * in_window
    lap_count = -(-seq_len // W)
    masked = jnp.concatenate([masked, jnp.zeros((lap_count * W - seq_len, 2 * HD), jnp.float32)], axis=0)
    kv_cache = lax.optimization_barrier(jnp.sum(masked.reshape(lap_count, W, 2 * HD), axis=0)).astype(jnp.bfloat16)
    return (lru_state, conv_state, kv_cache)

def reference(tokens, attn_in, lengths, norm_gain, attn_gain, w_x, conv_w, w_a, w_i, lru_decay, w_kv):

    def per_prompt(inputs):
        return one_prompt(norm_gain, attn_gain, w_x, conv_w, w_a, w_i, lru_decay, w_kv, inputs[0], inputs[1], inputs[2])
    lru_state, conv_state, kv_cache = lax.map(per_prompt, (tokens, attn_in, lengths))
    return (lru_state, conv_state, kv_cache)
```

```python
import heapq

import jax
import jax.numpy as jnp
import numpy as np
from jax import lax
from jax.experimental import pallas as pl
from jax.experimental.pallas import tpu as pltpu
from jax.sharding import Mesh
from jax.sharding import PartitionSpec as P

HD = 256
W = 2048
SEQ = ("seq_0", "seq_1")
BATCH = ("batch_0", "batch_1", "batch_2")
BATCH_SEQ = BATCH + SEQ
MESH_ID = pl.DeviceIdType.MESH

RING = {"x": 4, "y": 4, "z": 8}
PLANS = ((0, 5, "xyz"), (5, 4, "zxy"), (9, 4, "zyx"))
HEADS = 5
COLS = HEADS * HD
WIDE = 13 * 128
MAIN = 2048
LEFT = 512
HALO = 16


def phase_copies(share, phase):
    size = RING[PLANS[share][2][phase]]
    copies = []
    for step in range(size // 2):
        for way in (1, -1):
            for half in (0, 1):
                if step < size // 2 - 1 or half == (way < 0):
                    copies.append((share, phase, way, step, half))
    return copies


def gather_schedule():
    copies = [c for s in range(3) for p in range(3) for c in phase_copies(s, p)]
    index = {c: k for k, c in enumerate(copies)}
    waiting = {}
    for c in copies:
        share, phase, way, step, half = c
        if step:
            waiting[c] = {(share, phase, way, step - 1, half)}
        else:
            waiting[c] = set(phase_copies(share, phase - 1)) if phase else set()
    free, arrivals, order = {}, [], []

    def send(c, now):
        share, phase, way, _, _ = c
        volume = PLANS[share][1]
        for dim in PLANS[share][2][:phase]:
            volume *= RING[dim]
        link = (PLANS[share][2][phase], way)
        free[link] = max(now, free.get(link, 0.0)) + volume * 2048 / 46.6e3
        heapq.heappush(arrivals, (free[link] + 1.8, index[c]))
        order.append(("send", index[c]))

    for c in copies:
        if not waiting[c]:
            send(c, 0.0)
    while arrivals:
        now, k = heapq.heappop(arrivals)
        order.append(("recv", k))
        for c in copies:
            if copies[k] in waiting[c]:
                waiting[c].discard(copies[k])
                if not waiting[c]:
                    send(c, now)
    return copies, order


COPIES, ORDER = gather_schedule()


def exchange_kernel(
    block_ref,
    tokens_ref,
    tail_ref,
    length_ref,
    wide_ref,
    other_ref,
    halo_ref,
    other_halo_ref,
    other_length_ref,
    send_sem,
    recv_sem,
    pair_send,
    pair_recv,
    local_sem,
):
    z_lo = lax.axis_index("batch_0")
    core = lax.axis_index("batch_2")
    z_hi = lax.axis_index("seq_1")
    me = {"x": lax.axis_index("batch_1"), "y": lax.axis_index("seq_0"), "z": z_hi * 4 + z_lo}
    place = me["y"] * 2 + z_hi

    def toward(dim, way):
        spot = lax.rem(me[dim] + way + RING[dim], RING[dim])
        if dim == "x":
            return {"batch_1": spot}
        if dim == "y":
            return {"seq_0": spot}
        return {"batch_0": lax.rem(spot, 4), "seq_1": spot // 4}

    def at_place(spot):
        return {"seq_0": spot // 2, "seq_1": lax.rem(spot, 2)}

    partner = {"batch_2": 1 - core}
    after = at_place(lax.rem(place + 1, 8))
    before = at_place(lax.rem(place + 7, 8))
    barrier = pltpu.get_barrier_semaphore()
    friends = [toward(d, w) for d in "xyz" for w in (1, -1)] + [partner, after, before]
    for friend in friends:
        pl.semaphore_signal(barrier, inc=1, device_id=friend, device_id_type=MESH_ID)
    pl.semaphore_wait(barrier, len(friends))

    def remote(src, dst, sems, k, device):
        return pltpu.make_async_remote_copy(
            src_ref=src,
            dst_ref=dst,
            send_sem=sems[0].at[k],
            recv_sem=sems[1].at[k],
            device_id=device,
            device_id_type=MESH_ID,
        )

    pair = (pair_send, pair_recv)
    mine = wide_ref.at[me["z"], me["x"], pl.ds(2 * me["y"] + core, 1)]
    own = pltpu.make_async_copy(block_ref.at[pl.ds(core, 1)], mine, local_sem)
    own.start()
    given = remote(block_ref.at[pl.ds(1 - core, 1)], mine, pair, 0, partner)
    given.start()
    tail = remote(tail_ref, halo_ref, pair, 1, after)
    tail.start()
    length = remote(length_ref, other_length_ref, pair, 2, partner)
    length.start()
    rows = remote(tokens_ref, other_ref, pair, 3, partner)
    rows.start()

    def gather_copy(k):
        share, phase, way, step, half = COPIES[k]
        first, count, order = PLANS[share]
        dim = order[phase]
        spans = {d: pl.ds(0, RING[d]) for d in order[:phase]}
        spot = lax.rem(me[dim] - way * step + RING[dim], RING[dim])
        spans[dim] = pl.ds(spot, 1)
        for d in order[phase + 1 :]:
            spans[d] = pl.ds(me[d], 1)
        if "y" in order[:phase]:
            spans["y"] = pl.ds(4 * half, 4)
        else:
            y_at = spot if dim == "y" else me["y"]
            spans["y"] = pl.ds(2 * y_at + half, 1)
        piece = wide_ref.at[
            spans["z"], spans["x"], spans["y"], pl.ds(0, 8), pl.ds(first * 128, count * 128)
        ]
        return remote(piece, piece, (send_sem, recv_sem), k, toward(dim, way))

    own.wait()
    given.wait()
    started = {}
    seen = 0
    for what, k in ORDER:
        if what == "send":
            started[k] = gather_copy(k)
            started[k].start()
        else:
            started[k].wait_recv()
            seen += 1
            if seen == 30:
                tail.wait()
                passed = remote(halo_ref, other_halo_ref, pair, 4, partner)
                passed.start()
    for k in sorted(started):
        started[k].wait_send()
    length.wait()
    rows.wait()
    passed.wait()


def exchange(block, tokens, tail, length):
    feature_dim = tokens.shape[1]
    vmem = pl.BlockSpec(memory_space=pltpu.VMEM)
    hbm = pl.BlockSpec(memory_space=pl.ANY)
    return pl.pallas_call(
        exchange_kernel,
        out_shape=(
            jax.ShapeDtypeStruct((8, 4, 8, 8, WIDE), jnp.bfloat16),
            jax.ShapeDtypeStruct(tokens.shape, jnp.bfloat16),
            jax.ShapeDtypeStruct((4, feature_dim), jnp.bfloat16),
            jax.ShapeDtypeStruct((4, feature_dim), jnp.bfloat16),
            jax.ShapeDtypeStruct((8, 128), jnp.int32),
        ),
        in_specs=[hbm, hbm, vmem, vmem],
        out_specs=(vmem, hbm, vmem, vmem, vmem),
        scratch_shapes=[
            pltpu.SemaphoreType.DMA((len(COPIES),)),
            pltpu.SemaphoreType.DMA((len(COPIES),)),
            pltpu.SemaphoreType.DMA((5,)),
            pltpu.SemaphoreType.DMA((5,)),
            pltpu.SemaphoreType.DMA,
        ],
        compiler_params=pltpu.CompilerParams(collective_id=0, has_side_effects=True),
    )(block, tokens, tail, length)


def column_orders():
    order = np.zeros((640, 640), np.float32)
    for q in range(64):
        x, core, y, z_hi = q // 16, q // 8 % 2, q // 2 % 4, q % 2
        spot = x * 8 + y * 2 + core
        for i in range(10):
            if i < 8:
                order[10 * q + i, z_hi * 256 + spot * 8 + i] = 1
            else:
                order[10 * q + i, 512 + (i - 8) * 64 + z_hi * 32 + spot] = 1
    sort = np.zeros((256, 256), np.float32)
    for row in range(256):
        sort[row, row % 32 * 8 + row // 32] = 1
    return jnp.asarray(order, jnp.bfloat16), jnp.asarray(sort, jnp.bfloat16)


def f32_dot(a, b):
    return jnp.dot(a, b, preferred_element_type=jnp.float32)


def recurrence_kernel(
    info_ref,
    wide_ref,
    tokens_ref,
    other_ref,
    halo_ref,
    other_halo_ref,
    gain_ref,
    order_ref,
    sort_ref,
    conv_ref,
    rate_ref,
    wa_ref,
    wi_ref,
    out_ref,
    ordered,
    left,
    proj,
    gate_in,
):
    head = pl.program_id(0)
    place = info_ref[1]
    local_len = tokens_ref.shape[0]

    def place_rows(slot, start, raw):
        wide = raw.astype(jnp.float32)
        inverse = lax.rsqrt(jnp.mean(wide * wide, axis=-1, keepdims=True) + 1e-06)
        normed = (wide * inverse * gain_ref[...]).astype(jnp.bfloat16)
        rows = pl.ds(start, raw.shape[0])
        for g in range(4):
            moved = f32_dot(normed[:, 640 * g : 640 * (g + 1)], order_ref[...])
            moved = moved.astype(jnp.bfloat16)
            ordered[slot, rows, pl.ds(256 * g, 256)] = moved[:, :256]
            ordered[slot, rows, pl.ds(1024 + 256 * g, 256)] = moved[:, 256:512]
            ordered[slot, rows, pl.ds(MAIN + 128 * g, 128)] = moved[:, 512:]

    @pl.when(head == 0)
    def _():
        for slot, (body, edge) in enumerate(
            ((tokens_ref, halo_ref), (other_ref, other_halo_ref))
        ):
            edge_rows = edge[...].astype(jnp.float32)
            blank = jnp.zeros((HALO - 4, edge_rows.shape[1]), jnp.float32)
            place_rows(slot, 0, jnp.concatenate([blank, edge_rows], axis=0))

            def step(k, carry, slot=slot, body=body):
                start = pl.multiple_of(k * 64, 64)
                place_rows(slot, pl.multiple_of(HALO + start, 16), body[pl.ds(start, 64), :])
                return carry

            lax.fori_loop(0, local_len // 64, step, 0)
        for z in range(8):
            rest = wide_ref[256 * z : 256 * (z + 1), COLS:]
            sorted_rows = f32_dot(sort_ref[...], rest).astype(jnp.bfloat16)
            for r in range(2):
                for j in range(10):
                    unit = r * 10 + j
                    row = z % 4 * 128 + r * 64 + z // 4 * 32
                    left[row : row + 32, 128 * j : 128 * (j + 1)] = sorted_rows[
                        32 * (unit % 8) : 32 * (unit % 8) + 32,
                        128 * (unit // 8) : 128 * (unit // 8 + 1),
                    ]

    columns = pl.ds(pl.multiple_of(head * HD, HD), HD)
    after = (
        lax.broadcasted_iota(jnp.int32, (256, 256), 1)
        > lax.broadcasted_iota(jnp.int32, (256, 256), 0)
    ).astype(jnp.bfloat16)
    for slot in range(2):
        length = info_ref[2 + slot]
        total = f32_dot(ordered[slot, :, :MAIN], wide_ref[:, columns])
        total = total + f32_dot(ordered[slot, :, MAIN:], left[:, columns])
        x_proj = total.astype(jnp.bfloat16)
        shown = x_proj.astype(jnp.float32)
        proj[0:HALO, :] = jnp.where(place > 0, shown[:HALO], 0.0)
        proj[HALO:, :] = shown[HALO:]
        spots = place * local_len + lax.broadcasted_iota(jnp.int32, (8, local_len), 1)
        wanted = length - 3 + lax.broadcasted_iota(jnp.int32, (8, local_len), 0)
        picker = (spots == wanted).astype(jnp.bfloat16)
        picked = f32_dot(picker, x_proj[HALO:])
        conv_sum = conv_ref[0:1, :] * proj[pl.ds(HALO - 3, local_len), :]
        for offset in range(1, 4):
            conv_sum = conv_sum + conv_ref[offset : offset + 1, :] * proj[
                pl.ds(HALO - 3 + offset, local_len), :
            ]
        gate_in[...] = conv_sum.astype(jnp.bfloat16)
        log_total = jnp.zeros((1, HD), jnp.float32)
        state = jnp.zeros((1, HD), jnp.float32)
        for part in range(local_len // 256):
            x_conv = gate_in[256 * part : 256 * (part + 1), :]
            gate_a = f32_dot(x_conv, wa_ref[0])
            gate_i = f32_dot(x_conv, wi_ref[0])
            at = place * local_len + 256 * part
            at = at + lax.broadcasted_iota(jnp.int32, (256, 1), 0)
            valid = (at < length).astype(jnp.float32)
            log_rate = rate_ref[...] * (1.0 / (1.0 + jnp.exp(-gate_a)))
            y = 2.0 * log_rate
            series = 1.0 / 720.0 + y * (1.0 / 5040.0)
            for c in (1.0 / 120.0, 1.0 / 24.0, 1.0 / 6.0, 0.5, 1.0):
                series = c + y * series
            push = jnp.sqrt(-y * series) * (1.0 / (1.0 + jnp.exp(-gate_i)))
            push = push * x_conv.astype(jnp.float32) * valid
            kept = log_rate * valid
            high = kept.astype(jnp.bfloat16)
            low = (kept - high.astype(jnp.float32)).astype(jnp.bfloat16)
            later = f32_dot(after, high) + f32_dot(after, low)
            add = jnp.sum(jnp.exp(later) * push, axis=0, keepdims=True)
            log_part = jnp.sum(kept, axis=0, keepdims=True)
            state = jnp.exp(log_part) * state + add
            log_total = log_total + log_part
        out_ref[slot, 0:1, :] = log_total
        out_ref[slot, 1:2, :] = state
        out_ref[slot, 2:5, :] = picked[0:3]
        out_ref[slot, 5:8, :] = jnp.zeros((3, HD), jnp.float32)


def recurrence(info, wide, tokens, other, halo, other_halo, gain, conv_w, rate, w_a, w_i):
    order, sort = column_orders()
    vmem = pl.BlockSpec(memory_space=pltpu.VMEM)
    local_len, feature_dim = tokens.shape

    def of_head(h, info):
        return (0, HEADS * info[0] + h)

    def of_gate(h, info):
        return (HEADS * info[0] + h, 0, 0)

    return pl.pallas_call(
        recurrence_kernel,
        out_shape=jax.ShapeDtypeStruct((2, 8, COLS), jnp.float32),
        grid_spec=pltpu.PrefetchScalarGridSpec(
            num_scalar_prefetch=1,
            grid=(HEADS,),
            in_specs=[vmem] * 8
            + [
                pl.BlockSpec((4, HD), of_head),
                pl.BlockSpec((1, HD), of_head),
                pl.BlockSpec((1, HD, HD), of_gate),
                pl.BlockSpec((1, HD, HD), of_gate),
            ],
            out_specs=pl.BlockSpec((2, 8, HD), lambda h, info: (0, 0, h)),
            scratch_shapes=[
                pltpu.VMEM((2, HALO + local_len, feature_dim), jnp.bfloat16),
                pltpu.VMEM((LEFT, COLS), jnp.bfloat16),
                pltpu.VMEM((HALO + local_len, HD), jnp.float32),
                pltpu.VMEM((local_len, HD), jnp.bfloat16),
            ],
        ),
        compiler_params=pltpu.CompilerParams(
            dimension_semantics=("arbitrary",), vmem_limit_bytes=60 * 2**20
        ),
        cost_estimate=pl.CostEstimate(
            flops=10**10, bytes_accessed=16 * 2**20, transcendentals=10**7
        ),
    )(info, wide, tokens, other, halo, other_halo, gain, order, sort, conv_w, rate, w_a, w_i)


def collect_kernel(parts_ref, state_ref, conv_ref, arrived, send_sem, recv_sem, local_sem):
    core = lax.axis_index("batch_2")
    y = lax.axis_index("seq_0")
    z_hi = lax.axis_index("seq_1")
    place = y * 2 + z_hi

    def device(spot, c):
        return {"batch_2": c, "seq_0": spot // 2, "seq_1": lax.rem(spot, 2)}

    barrier = pltpu.get_barrier_semaphore()
    for turn in range(8):
        for flip in range(2):
            if turn or flip:
                friend = device(lax.rem(place + turn, 8), lax.rem(core + flip, 2))
                pl.semaphore_signal(barrier, inc=1, device_id=friend, device_id_type=MESH_ID)
    pl.semaphore_wait(barrier, 15)

    def part_copy(slot, k):
        return pltpu.make_async_remote_copy(
            src_ref=parts_ref.at[slot, k],
            dst_ref=arrived.at[place],
            send_sem=send_sem.at[slot * 4 + k],
            recv_sem=recv_sem.at[place],
            device_id=device(4 * core + k, lax.rem(core + slot, 2)),
            device_id_type=MESH_ID,
        )

    def is_own(slot, k):
        return jnp.logical_and(slot == 0, place == 4 * core + k)

    for slot in range(2):
        for k in range(4):
            own = is_own(slot, k)

            @pl.when(jnp.logical_not(own))
            def _(slot=slot, k=k):
                part_copy(slot, k).start()

            @pl.when(own)
            def _(slot=slot, k=k):
                copy = pltpu.make_async_copy(parts_ref.at[slot, k], arrived.at[place], local_sem)
                copy.start()
                copy.wait()

    near = core == place // 4
    for spot in range(8):

        @pl.when(jnp.logical_not(jnp.logical_and(near, place == spot)))
        def _(spot=spot):
            pltpu.make_async_remote_copy(
                src_ref=parts_ref.at[0, 0],
                dst_ref=arrived.at[spot],
                send_sem=send_sem.at[0],
                recv_sem=recv_sem.at[spot],
                device_id={"batch_2": 1 - core},
                device_id_type=MESH_ID,
            ).wait_recv()

    state = jnp.zeros((1, state_ref.shape[1]), jnp.float32)
    conv = jnp.zeros((3, state_ref.shape[1]), jnp.float32)
    for spot in range(8):
        state = jnp.exp(arrived[spot, 0:1]) * state + arrived[spot, 1:2]
        conv = conv + arrived[spot, 2:5]
    state_ref[...] = state
    conv_ref[...] = conv.astype(jnp.bfloat16)
    for slot in range(2):
        for k in range(4):

            @pl.when(jnp.logical_not(is_own(slot, k)))
            def _(slot=slot, k=k):
                part_copy(slot, k).wait_send()


def collect(parts):
    vmem = pl.BlockSpec(memory_space=pltpu.VMEM)
    width = parts.shape[-1]
    return pl.pallas_call(
        collect_kernel,
        out_shape=(
            jax.ShapeDtypeStruct((1, width), jnp.float32),
            jax.ShapeDtypeStruct((3, width), jnp.bfloat16),
        ),
        in_specs=[pl.BlockSpec(memory_space=pl.ANY)],
        out_specs=(vmem, vmem),
        scratch_shapes=[
            pltpu.VMEM((8, 8, width), jnp.float32),
            pltpu.SemaphoreType.DMA((8,)),
            pltpu.SemaphoreType.DMA((8,)),
            pltpu.SemaphoreType.DMA,
        ],
        compiler_params=pltpu.CompilerParams(collective_id=1, has_side_effects=True),
    )(parts)


def rms_norm(values, gain_vec):
    widened = values.astype(jnp.float32)
    inverse = lax.rsqrt(jnp.mean(widened * widened, axis=-1, keepdims=True) + 1e-06)
    return (widened * inverse * gain_vec).astype(jnp.bfloat16)


def rotate_keys(key_rows, positions):
    quarter = key_rows.shape[-1] // 4
    spacing = jnp.exp(-jnp.log(10000.0) * jnp.arange(quarter, dtype=jnp.float32) / quarter)
    angles = positions.astype(jnp.float32)[:, None] * spacing[None, :]
    cosine_rows = jnp.cos(angles)
    sine_rows = jnp.sin(angles)
    first_part = key_rows[:, :quarter]
    second_part = key_rows[:, quarter : 2 * quarter]
    return jnp.concatenate(
        [
            first_part * cosine_rows - second_part * sine_rows,
            second_part * cosine_rows + first_part * sine_rows,
            key_rows[:, 2 * quarter :],
        ],
        axis=1,
    )


def window_cache(attn_in, length, attn_gain, w_kv, positions):
    attn_normed = rms_norm(attn_in, attn_gain)
    kv_full = jnp.dot(attn_normed, w_kv, preferred_element_type=jnp.float32)
    kv_rows = jnp.concatenate(
        [rotate_keys(kv_full[:, :HD], positions), kv_full[:, HD:]], axis=1
    ).astype(jnp.bfloat16)
    in_window = ((positions >= length - W) & (positions < length)).astype(jnp.float32)[:, None]
    masked = kv_rows.astype(jnp.float32) * in_window
    arrived = lax.all_to_all(
        masked.astype(jnp.bfloat16), SEQ, split_axis=1, concat_axis=0, tiled=True
    )
    total_len = arrived.shape[0]
    lap_count = -(-total_len // W)
    widened = arrived.astype(jnp.float32)
    return jnp.sum(widened.reshape(lap_count, W, arrived.shape[1]), axis=0).astype(jnp.bfloat16)


def transport_block(w_rows):
    halves = w_rows.reshape(10, 2, COLS).transpose(1, 0, 2)
    rest = halves[:, 8:].reshape(2, 20, 128)
    rest = jnp.concatenate([rest, jnp.zeros((2, 4, 128), rest.dtype)], axis=1)
    rest = rest.reshape(2, 3, 8, 128).transpose(0, 2, 1, 3).reshape(2, 8, 384)
    return jnp.concatenate([halves[:, :8], rest], axis=2)


def on_device(
    tokens, attn_in, lengths, norm_gain, attn_gain, w_x, conv_w, w_a, w_i, lru_decay, w_kv
):
    local_len = tokens.shape[1]
    place = lax.axis_index(SEQ)
    core = lax.axis_index("batch_2")
    length = lengths[0]
    wide, other, halo, other_halo, other_length = exchange(
        transport_block(w_x),
        tokens[0],
        tokens[0, local_len - 4 :],
        jnp.broadcast_to(length, (8, 128)),
    )
    positions = place * local_len + jnp.arange(local_len, dtype=jnp.int32)
    kv_cache = window_cache(attn_in[0], length, attn_gain, w_kv, positions)
    info = jnp.stack([core, place, length, other_length[0, 0]])
    rate = -8.0 * jax.nn.softplus(-lru_decay)
    sums = recurrence(
        info,
        wide.reshape(MAIN, WIDE),
        tokens[0],
        other,
        halo,
        other_halo,
        norm_gain[None],
        conv_w,
        rate[None],
        w_a,
        w_i,
    )
    parts = sums.reshape(2, 8, 4, COLS // 4).transpose(0, 2, 1, 3)
    lru_state, conv_state = collect(parts)
    return (lru_state, conv_state[None], kv_cache[None])


def solution(mesh):
    split = Mesh(mesh.devices.reshape(4, 4, 2, 4, 2), BATCH_SEQ)
    in_specs = (
        P(BATCH, SEQ, None),
        P(BATCH, SEQ, None),
        P(BATCH),
        P(),
        P(),
        P(BATCH_SEQ, None),
        P(),
        P(),
        P(),
        P(),
        P(),
    )
    out_specs = (P(BATCH, SEQ), P(BATCH, None, SEQ), P(BATCH, None, SEQ))
    return jax.shard_map(
        on_device, mesh=split, in_specs=in_specs, out_specs=out_specs, check_vma=False
    )
```

```python
import heapq

import jax
import jax.numpy as jnp
import numpy as np
from jax import lax
from jax.experimental import pallas as pl
from jax.experimental.pallas import tpu as pltpu
from jax.sharding import Mesh
from jax.sharding import PartitionSpec as P

HD = 256
W = 2048
SEQ = ("seq_0", "seq_1")
BATCH = ("batch_0", "batch_1", "batch_2")
BATCH_SEQ = BATCH + SEQ
MESH_ID = pl.DeviceIdType.MESH

RING = {"x": 4, "y": 4, "z": 8}
PLANS = ((0, 5, "xyz"), (5, 4, "zxy"), (9, 4, "zyx"))
HEADS = 5
COLS = HEADS * HD
WIDE = 13 * 128
MAIN = 2048
LEFT = 512
HALO = 16


def phase_copies(share, phase):
    size = RING[PLANS[share][2][phase]]
    copies = []
    for step in range(size // 2):
        for way in (1, -1):
            for half in (0, 1):
                if step < size // 2 - 1 or half == (way < 0):
                    copies.append((share, phase, way, step, half))
    return copies


def gather_schedule():
    copies = [c for s in range(3) for p in range(3) for c in phase_copies(s, p)]
    index = {c: k for k, c in enumerate(copies)}
    waiting = {}
    for c in copies:
        share, phase, way, step, half = c
        if step:
            waiting[c] = {(share, phase, way, step - 1, half)}
        else:
            waiting[c] = set(phase_copies(share, phase - 1)) if phase else set()
    free, arrivals, order = {}, [], []

    def send(c, now):
        share, phase, way, _, _ = c
        volume = PLANS[share][1]
        for dim in PLANS[share][2][:phase]:
            volume *= RING[dim]
        link = (PLANS[share][2][phase], way)
        free[link] = max(now, free.get(link, 0.0)) + volume * 2048 / 46.6e3
        heapq.heappush(arrivals, (free[link] + 1.8, index[c]))
        order.append(("send", index[c], now))

    for c in copies:
        if not waiting[c]:
            send(c, 0.0)
    while arrivals:
        now, k = heapq.heappop(arrivals)
        order.append(("recv", k, now))
        for c in copies:
            if copies[k] in waiting[c]:
                waiting[c].discard(copies[k])
                if not waiting[c]:
                    send(c, now)
    return copies, order


COPIES, ORDER = gather_schedule()


def column_orders():
    order = np.zeros((640, 640), np.float32)
    for q in range(64):
        x, core, y, z_hi = q // 16, q // 8 % 2, q // 2 % 4, q % 2
        spot = x * 8 + y * 2 + core
        for i in range(10):
            if i < 8:
                order[10 * q + i, z_hi * 256 + spot * 8 + i] = 1
            else:
                order[10 * q + i, 512 + (i - 8) * 64 + z_hi * 32 + spot] = 1
    sort = np.zeros((256, 256), np.float32)
    for row in range(256):
        sort[row, row % 32 * 8 + row // 32] = 1
    return jnp.asarray(order, jnp.bfloat16), jnp.asarray(sort, jnp.bfloat16)


def f32_dot(a, b):
    return jnp.dot(a, b, preferred_element_type=jnp.float32)


def normed_rows(raw, gain):
    wide = raw.astype(jnp.float32)
    inverse = lax.rsqrt(jnp.mean(wide * wide, axis=-1, keepdims=True) + 1e-06)
    return (wide * inverse * gain).astype(jnp.bfloat16)


def sigmoid(values):
    return 1.0 / (1.0 + jnp.exp(-values))


def prefill_kernel(
    block_hbm,
    tokens_hbm,
    attn_hbm,
    wkv_hbm,
    wa_hbm,
    wi_hbm,
    tail_ref,
    length_ref,
    gain_ref,
    attn_gain_ref,
    order_ref,
    sort_ref,
    conv_ref,
    rate_ref,
    cos_ref,
    sin_ref,
    state_out,
    conv_out,
    cache_out,
    wide,
    rows,
    ordered,
    left,
    proj,
    gate_in,
    attn,
    wkv,
    gates,
    halo,
    other_length,
    sums,
    parts,
    arrived,
    packed,
    cached,
    send_sem,
    recv_sem,
    pair_send,
    pair_recv,
    local_sem,
    part_send,
    part_recv,
    kv_send,
    kv_recv,
):
    z_lo = lax.axis_index("batch_0")
    core = lax.axis_index("batch_2")
    z_hi = lax.axis_index("seq_1")
    me = {"x": lax.axis_index("batch_1"), "y": lax.axis_index("seq_0"), "z": z_hi * 4 + z_lo}
    place = me["y"] * 2 + z_hi
    local_len = tokens_hbm.shape[0]
    span = HALO + local_len

    def toward(dim, way):
        spot = lax.rem(me[dim] + way + RING[dim], RING[dim])
        if dim == "x":
            return {"batch_1": spot}
        if dim == "y":
            return {"seq_0": spot}
        return {"batch_0": lax.rem(spot, 4), "seq_1": spot // 4}

    def beside(spot, c):
        return {"batch_2": c, "seq_0": spot // 2, "seq_1": lax.rem(spot, 2)}

    partner = {"batch_2": 1 - core}
    after = beside(lax.rem(place + 1, 8), core)

    barrier = pltpu.get_barrier_semaphore()
    friends = [toward(d, w) for d in "xz" for w in (1, -1)]
    for turn in range(8):
        for flip in range(2):
            if turn or flip:
                friends.append(beside(lax.rem(place + turn, 8), lax.rem(core + flip, 2)))
    for friend in friends:
        pl.semaphore_signal(barrier, inc=1, device_id=friend, device_id_type=MESH_ID)

    def remote(src, dst, sems, k, device):
        return pltpu.make_async_remote_copy(
            src_ref=src,
            dst_ref=dst,
            send_sem=sems[0].at[k],
            recv_sem=sems[1].at[k],
            device_id=device,
            device_id_type=MESH_ID,
        )

    mine = wide.at[me["z"], me["x"], pl.ds(2 * me["y"] + core, 1)]
    own_heads = pl.ds(HEADS * core, HEADS)
    fetches = [
        pltpu.make_async_copy(src, dst, local_sem.at[k])
        for k, (src, dst) in enumerate(
            (
                (tokens_hbm, rows.at[0]),
                (block_hbm.at[pl.ds(core, 1)], mine),
                (attn_hbm, attn),
                (wkv_hbm, wkv),
                (wa_hbm.at[own_heads], gates.at[0]),
                (wi_hbm.at[own_heads], gates.at[1]),
            )
        )
    ]
    for fetch in fetches:
        fetch.start()

    def place_rows(slot, start, raw):
        normed = normed_rows(raw, gain_ref[...])
        at = pl.ds(slot * span + start, raw.shape[0])
        for g in range(4):
            moved = f32_dot(normed[:, 640 * g : 640 * (g + 1)], order_ref[...])
            moved = moved.astype(jnp.bfloat16)
            ordered[at, pl.ds(256 * g, 256)] = moved[:, :256]
            ordered[at, pl.ds(1024 + 256 * g, 256)] = moved[:, 256:512]
            ordered[at, pl.ds(MAIN + 128 * g, 128)] = moved[:, 512:]

    def body_rows(slot, k):
        place_rows(slot, HALO + 256 * k, rows[slot, 256 * k : 256 * (k + 1), :])

    def edge_rows(slot):
        edge = halo[slot].astype(jnp.float32)
        blank = jnp.zeros((HALO - 4, edge.shape[1]), jnp.float32)
        place_rows(slot, 0, jnp.concatenate([blank, edge], axis=0))

    length = length_ref[0:1, 0:1]

    def cache_rows(k):
        tops = []
        lane = lax.broadcasted_iota(jnp.int32, (128, 128), 1)
        for start in (128 * k, 256 + 128 * k):
            normed = normed_rows(attn[start : start + 128, :], attn_gain_ref[...])
            kv = f32_dot(normed, wkv[...])
            turned = kv[:, :128] * cos_ref[start : start + 128, :]
            turned = turned + pltpu.roll(kv[:, :128], 64, 1) * sin_ref[start : start + 128, :]
            kv = jnp.concatenate([turned, kv[:, 128:]], axis=1).astype(jnp.bfloat16)
            at = place * local_len + start + lax.broadcasted_iota(jnp.int32, (128, 1), 0)
            inside = ((at >= length - W) & (at < length)).astype(jnp.float32)
            tops.append(kv.astype(jnp.float32) * inside)
        for t in range(4):
            upper = tops[0][:, 128 * t : 128 * (t + 1)]
            lower = tops[1][:, 128 * t : 128 * (t + 1)]
            even = jnp.where(lane < 64, upper, pltpu.roll(lower, 64, 1))
            odd = jnp.where(lane < 64, pltpu.roll(upper, 64, 1), lower)
            packed[2 * t, 128 * k : 128 * (k + 1), :] = even.astype(jnp.bfloat16)
            packed[2 * t + 1, 128 * k : 128 * (k + 1), :] = odd.astype(jnp.bfloat16)

    fetches[0].wait()
    body_rows(0, 0)
    pl.semaphore_wait(barrier, len(friends))

    pair = (pair_send, pair_recv)
    given = remote(block_hbm.at[pl.ds(1 - core, 1)], mine, pair, 0, partner)
    given.start()
    tail = remote(tail_ref, halo.at[0], pair, 1, after)
    tail.start()
    length_copy = remote(length_ref, other_length, pair, 2, partner)
    length_copy.start()
    rows_copy = remote(tokens_hbm, rows.at[1], pair, 3, partner)
    rows_copy.start()
    passed = remote(halo.at[0], halo.at[1], pair, 4, partner)

    def gather_copy(k):
        share, phase, way, step, half = COPIES[k]
        first, count, order = PLANS[share]
        dim = order[phase]
        spans = {d: pl.ds(0, RING[d]) for d in order[:phase]}
        spot = lax.rem(me[dim] - way * step + RING[dim], RING[dim])
        spans[dim] = pl.ds(spot, 1)
        for d in order[phase + 1 :]:
            spans[d] = pl.ds(me[d], 1)
        if "y" in order[:phase]:
            spans["y"] = pl.ds(4 * half, 4)
        else:
            y_at = spot if dim == "y" else me["y"]
            spans["y"] = pl.ds(2 * y_at + half, 1)
        piece = wide.at[
            spans["z"], spans["x"], spans["y"], pl.ds(0, 8), pl.ds(first * 128, count * 128)
        ]
        return remote(piece, piece, (send_sem, recv_sem), k, toward(dim, way))

    def start_other():
        rows_copy.wait()
        body_rows(1, 0)

    def pass_halo():
        tail.wait()
        passed.start()

    def start_cache():
        fetches[2].wait()
        fetches[3].wait()
        cache_rows(0)

    def end_halo():
        passed.wait()
        edge_rows(1)

    tasks = [
        (6.0, pass_halo),
        (10.0, lambda: body_rows(0, 1)),
        (14.0, start_other),
        (17.0, lambda: body_rows(1, 1)),
        (20.0, start_cache),
        (23.0, lambda: cache_rows(1)),
        (26.0, lambda: edge_rows(0)),
        (28.0, end_halo),
    ]
    fetches[1].wait()
    given.wait()
    started = {}
    for what, k, when in ORDER:
        if what == "send":
            started[k] = gather_copy(k)
            started[k].start()
        else:
            while tasks and tasks[0][0] <= when:
                tasks.pop(0)[1]()
            started[k].wait_recv()
    for _, task in tasks:
        task()

    def kv_copy(turn):
        spot = lax.rem(place + turn, 8)
        return pltpu.make_async_remote_copy(
            src_ref=packed.at[spot],
            dst_ref=cached.at[place],
            send_sem=kv_send.at[turn],
            recv_sem=kv_recv.at[turn],
            device_id=beside(spot, core),
            device_id_type=MESH_ID,
        )

    kv_copies = [kv_copy(turn) for turn in range(1, 8)]
    for copy in kv_copies:
        copy.start()
    fetches[4].wait()
    fetches[5].wait()
    length_copy.wait()

    for z in range(8):
        rest = wide[z, :, :, :, COLS:].reshape(256, WIDE - COLS)
        sorted_rows = f32_dot(sort_ref[...], rest).astype(jnp.bfloat16)
        for r in range(2):
            for j in range(10):
                unit = r * 10 + j
                row = z % 4 * 128 + r * 64 + z // 4 * 32
                left[row : row + 32, 128 * j : 128 * (j + 1)] = sorted_rows[
                    32 * (unit % 8) : 32 * (unit % 8) + 32,
                    128 * (unit // 8) : 128 * (unit // 8 + 1),
                ]

    later_rows = (
        lax.broadcasted_iota(jnp.int32, (256, 256), 1)
        > lax.broadcasted_iota(jnp.int32, (256, 256), 0)
    ).astype(jnp.bfloat16)
    lengths = (length, other_length[0:1, 0:1])

    def head_step(head, carry):
        columns = pl.ds(pl.multiple_of(head * HD, HD), HD)
        channels = pl.ds(pl.multiple_of((HEADS * core + head) * HD, HD), HD)
        weight = wide[:, :, :, :, columns].reshape(MAIN, HD)
        total = f32_dot(ordered[:, :MAIN], weight)
        total = total + f32_dot(ordered[:, MAIN:], left[:, columns])
        proj[...] = total.astype(jnp.bfloat16).astype(jnp.float32)
        taps = conv_ref[:, channels]
        rate = rate_ref[:, channels]
        for slot in range(2):
            base = slot * span
            edge = proj[base : base + HALO, :]
            proj[base : base + HALO, :] = jnp.where(place > 0, edge, 0.0)
            spots = place * local_len + lax.broadcasted_iota(jnp.int32, (8, local_len), 1)
            wanted = lengths[slot] - 3 + lax.broadcasted_iota(jnp.int32, (8, local_len), 0)
            picker = (spots == wanted).astype(jnp.bfloat16)
            picked = f32_dot(picker, proj[base + HALO : base + span, :].astype(jnp.bfloat16))
            log_total = jnp.zeros((1, HD), jnp.float32)
            state = jnp.zeros((1, HD), jnp.float32)
            for part in range(local_len // 256):
                first = base + HALO - 3 + 256 * part
                conv_sum = taps[0:1, :] * proj[pl.ds(first, 256), :]
                for offset in range(1, 4):
                    tap = taps[offset : offset + 1, :]
                    conv_sum = conv_sum + tap * proj[pl.ds(first + offset, 256), :]
                x_conv = conv_sum.astype(jnp.bfloat16)
                gate_a = f32_dot(x_conv, gates[0, head])
                gate_i = f32_dot(x_conv, gates[1, head])
                at = place * local_len + 256 * part
                at = at + lax.broadcasted_iota(jnp.int32, (256, 1), 0)
                valid = (at < lengths[slot]).astype(jnp.float32)
                log_rate = rate * sigmoid(gate_a)
                y = 2.0 * log_rate
                series = 1.0 / 720.0 + y * (1.0 / 5040.0)
                for c in (1.0 / 120.0, 1.0 / 24.0, 1.0 / 6.0, 0.5, 1.0):
                    series = c + y * series
                push = jnp.sqrt(-y * series) * sigmoid(gate_i)
                push = push * x_conv.astype(jnp.float32) * valid
                kept = log_rate * valid
                high = kept.astype(jnp.bfloat16)
                low = (kept - high.astype(jnp.float32)).astype(jnp.bfloat16)
                later = f32_dot(later_rows, high) + f32_dot(later_rows, low)
                add = jnp.sum(jnp.exp(later) * push, axis=0, keepdims=True)
                log_part = jnp.sum(kept, axis=0, keepdims=True)
                state = jnp.exp(log_part) * state + add
                log_total = log_total + log_part
            sums[slot, 0:1, columns] = log_total
            sums[slot, 1:2, columns] = state
            sums[slot, 2:5, columns] = picked[0:3]
        return carry

    sums[...] = jnp.zeros_like(sums)
    lax.fori_loop(0, HEADS, head_step, 0)

    for slot in range(2):
        for k in range(4):
            whole = sums[slot]
            if k:
                whole = pltpu.roll(whole, COLS - 320 * k, 1)
            parts[slot, k] = whole[:, :384]

    def part_copy(slot, k):
        return pltpu.make_async_remote_copy(
            src_ref=parts.at[slot, k],
            dst_ref=arrived.at[place],
            send_sem=part_send.at[slot * 4 + k],
            recv_sem=part_recv.at[place],
            device_id=beside(4 * core + k, lax.rem(core + slot, 2)),
            device_id_type=MESH_ID,
        )

    def is_own(slot, k):
        return jnp.logical_and(slot == 0, place == 4 * core + k)

    for slot in range(2):
        for k in range(4):

            @pl.when(jnp.logical_not(is_own(slot, k)))
            def _(slot=slot, k=k):
                part_copy(slot, k).start()

    for k in range(4):

        @pl.when(is_own(0, k))
        def _(k=k):
            arrived[place] = parts[0, k]

    cached[place] = packed[place]
    for copy in kv_copies:
        copy.wait()
    for k in range(4):
        both = cached[k].astype(jnp.float32) + cached[k + 4].astype(jnp.float32)
        cache_out[512 * k : 512 * k + 256, :] = both[:, :64].astype(jnp.bfloat16)
        turned = pltpu.roll(both, 64, 1)
        cache_out[512 * k + 256 : 512 * k + 512, :] = turned[:, :64].astype(jnp.bfloat16)

    near = core == place // 4
    for spot in range(8):

        @pl.when(jnp.logical_not(jnp.logical_and(near, place == spot)))
        def _(spot=spot):
            pltpu.make_async_remote_copy(
                src_ref=parts.at[0, 0],
                dst_ref=arrived.at[spot],
                send_sem=part_send.at[0],
                recv_sem=part_recv.at[spot],
                device_id=partner,
                device_id_type=MESH_ID,
            ).wait_recv()

    width = state_out.shape[1]
    state = jnp.zeros((1, width), jnp.float32)
    conv = jnp.zeros((3, width), jnp.float32)
    for spot in range(8):
        state = jnp.exp(arrived[spot, 0:1, :width]) * state + arrived[spot, 1:2, :width]
        conv = conv + arrived[spot, 2:5, :width]
    state_out[...] = state
    conv_out[...] = conv.astype(jnp.bfloat16)
    for slot in range(2):
        for k in range(4):

            @pl.when(jnp.logical_not(is_own(slot, k)))
            def _(slot=slot, k=k):
                part_copy(slot, k).wait_send()

    for k in sorted(started):
        started[k].wait_send()


def prefill(block, tokens, attn_in, w_kv, w_a, w_i, *small):
    order, sort = column_orders()
    local_len, feature_dim = tokens.shape
    tail, length, gain, attn_gain, conv_w, rate, cosine, sine = small
    vmem = pl.BlockSpec(memory_space=pltpu.VMEM)
    hbm = pl.BlockSpec(memory_space=pl.ANY)
    dma = pltpu.SemaphoreType.DMA
    span = HALO + local_len
    return pl.pallas_call(
        prefill_kernel,
        out_shape=(
            jax.ShapeDtypeStruct((1, feature_dim // 8), jnp.float32),
            jax.ShapeDtypeStruct((3, feature_dim // 8), jnp.bfloat16),
            jax.ShapeDtypeStruct((W, 64), jnp.bfloat16),
        ),
        in_specs=[hbm] * 6 + [vmem] * 10,
        out_specs=(vmem, vmem, vmem),
        scratch_shapes=[
            pltpu.VMEM((8, 4, 8, 8, WIDE), jnp.bfloat16),
            pltpu.VMEM((2, local_len, feature_dim), jnp.bfloat16),
            pltpu.VMEM((2 * span, feature_dim), jnp.bfloat16),
            pltpu.VMEM((LEFT, COLS), jnp.bfloat16),
            pltpu.VMEM((2 * span, HD), jnp.float32),
            pltpu.VMEM((local_len, HD), jnp.bfloat16),
            pltpu.VMEM((local_len, feature_dim), jnp.bfloat16),
            pltpu.VMEM(w_kv.shape, jnp.bfloat16),
            pltpu.VMEM((2, HEADS, HD, HD), jnp.bfloat16),
            pltpu.VMEM((2, 4, feature_dim), jnp.bfloat16),
            pltpu.VMEM((8, 128), jnp.int32),
            pltpu.VMEM((2, 8, COLS), jnp.float32),
            pltpu.VMEM((2, 4, 8, 384), jnp.float32),
            pltpu.VMEM((8, 8, 384), jnp.float32),
            pltpu.VMEM((8, local_len // 2, 128), jnp.bfloat16),
            pltpu.VMEM((8, local_len // 2, 128), jnp.bfloat16),
            dma((len(COPIES),)),
            dma((len(COPIES),)),
            dma((5,)),
            dma((5,)),
            dma((6,)),
            dma((8,)),
            dma((8,)),
            dma((8,)),
            dma((8,)),
        ],
        compiler_params=pltpu.CompilerParams(
            collective_id=0, has_side_effects=True, vmem_limit_bytes=63 * 2**20
        ),
    )(
        block, tokens, attn_in, w_kv, w_a, w_i, tail, length, gain, attn_gain, order, sort,
        conv_w, rate, cosine, sine,
    )


def transport_block(w_rows):
    halves = w_rows.reshape(10, 2, COLS).transpose(1, 0, 2)
    rest = halves[:, 8:].reshape(2, 20, 128)
    rest = jnp.concatenate([rest, jnp.zeros((2, 4, 128), rest.dtype)], axis=1)
    rest = rest.reshape(2, 3, 8, 128).transpose(0, 2, 1, 3).reshape(2, 8, 384)
    return jnp.concatenate([halves[:, :8], rest], axis=2)


def on_device(
    tokens, attn_in, lengths, norm_gain, attn_gain, w_x, conv_w, w_a, w_i, lru_decay, w_kv
):
    local_len = tokens.shape[1]
    place = lax.axis_index(SEQ)
    positions = place * local_len + jnp.arange(local_len, dtype=jnp.int32)
    spacing = jnp.exp(-jnp.log(10000.0) * jnp.arange(64, dtype=jnp.float32) / 64)
    angles = positions.astype(jnp.float32)[:, None] * spacing[None, :]
    cosine, sine = jnp.cos(angles), jnp.sin(angles)
    lru_state, conv_state, kv_cache = prefill(
        transport_block(w_x),
        tokens[0],
        attn_in[0],
        w_kv,
        w_a,
        w_i,
        tokens[0, local_len - 4 :],
        jnp.broadcast_to(lengths[0], (8, 128)),
        norm_gain[None],
        attn_gain[None],
        conv_w,
        (-8.0 * jax.nn.softplus(-lru_decay))[None],
        jnp.concatenate([cosine, cosine], axis=1),
        jnp.concatenate([-sine, sine], axis=1),
    )
    return (lru_state, conv_state[None], kv_cache[None])


def solution(mesh):
    split = Mesh(mesh.devices.reshape(4, 4, 2, 4, 2), BATCH_SEQ)
    in_specs = (
        P(BATCH, SEQ, None),
        P(BATCH, SEQ, None),
        P(BATCH),
        P(),
        P(),
        P(BATCH_SEQ, None),
        P(),
        P(),
        P(),
        P(),
        P(),
    )
    out_specs = (P(BATCH, SEQ), P(BATCH, None, SEQ), P(BATCH, None, SEQ))
    return jax.shard_map(
        on_device, mesh=split, in_specs=in_specs, out_specs=out_specs, check_vma=False
    )
```

```python
import heapq

import jax
import jax.numpy as jnp
import numpy as np
from jax import lax
from jax.experimental import pallas as pl
from jax.experimental.pallas import tpu as pltpu
from jax.sharding import Mesh
from jax.sharding import PartitionSpec as P

HD = 256
W = 2048
SEQ = ("seq_0", "seq_1")
BATCH = ("batch_0", "batch_1", "batch_2")
BATCH_SEQ = BATCH + SEQ
MESH_ID = pl.DeviceIdType.MESH

RING = {"x": 4, "y": 4, "z": 8}
PLANS = ((0, 5, "xyz"), (5, 4, "zxy"), (9, 4, "zyx"))
HEADS = 5
COLS = HEADS * HD
WIDE = 13 * 128
MAIN = 2048
LEFT = 512
HALO = 16


def phase_copies(share, phase):
    size = RING[PLANS[share][2][phase]]
    copies = []
    for step in range(size // 2):
        for way in (1, -1):
            for half in (0, 1):
                if step < size // 2 - 1 or half == (way < 0):
                    copies.append((share, phase, way, step, half))
    return copies


def gather_schedule():
    copies = [c for s in range(3) for p in range(3) for c in phase_copies(s, p)]
    index = {c: k for k, c in enumerate(copies)}
    waiting = {}
    for c in copies:
        share, phase, way, step, half = c
        if step:
            waiting[c] = {(share, phase, way, step - 1, half)}
        else:
            waiting[c] = set(phase_copies(share, phase - 1)) if phase else set()
    free, arrivals, order = {}, [], []

    def send(c, now):
        share, phase, way, _, _ = c
        volume = PLANS[share][1]
        for dim in PLANS[share][2][:phase]:
            volume *= RING[dim]
        link = (PLANS[share][2][phase], way)
        free[link] = max(now, free.get(link, 0.0)) + volume * 2048 / 46.6e3
        heapq.heappush(arrivals, (free[link] + 1.8, index[c]))
        order.append(("send", index[c], now))

    for c in copies:
        if not waiting[c]:
            send(c, 0.0)
    while arrivals:
        now, k = heapq.heappop(arrivals)
        order.append(("recv", k, now))
        for c in copies:
            if copies[k] in waiting[c]:
                waiting[c].discard(copies[k])
                if not waiting[c]:
                    send(c, now)
    return copies, order


COPIES, ORDER = gather_schedule()


def column_orders():
    order = np.zeros((640, 640), np.float32)
    for q in range(64):
        x, core, y, z_hi = q // 16, q // 8 % 2, q // 2 % 4, q % 2
        spot = x * 8 + y * 2 + core
        for i in range(10):
            if i < 8:
                order[10 * q + i, z_hi * 256 + spot * 8 + i] = 1
            else:
                order[10 * q + i, 512 + (i - 8) * 64 + z_hi * 32 + spot] = 1
    sort = np.zeros((256, 256), np.float32)
    for row in range(256):
        sort[row, row % 32 * 8 + row // 32] = 1
    return jnp.asarray(order, jnp.bfloat16), jnp.asarray(sort, jnp.bfloat16)


def f32_dot(a, b):
    return jnp.dot(a, b, preferred_element_type=jnp.float32)


def normed_rows(raw, gain):
    wide = raw.astype(jnp.float32)
    inverse = lax.rsqrt(jnp.mean(wide * wide, axis=-1, keepdims=True) + 1e-06)
    return (wide * inverse * gain).astype(jnp.bfloat16)


def sigmoid(values):
    return 1.0 / (1.0 + jnp.exp(-values))


def prefill_kernel(
    length_in,
    tokens_hbm,
    attn_hbm,
    wkv_hbm,
    wa_hbm,
    wi_hbm,
    shard_ref,
    gain_ref,
    attn_gain_ref,
    decay_ref,
    conv_ref,
    order_ref,
    sort_ref,
    trig_ref,
    arrived,
    cached,
    wide,
    rows,
    ordered,
    left,
    proj_even,
    proj_odd,
    attn,
    wkv,
    gates,
    halo,
    tail_rows,
    lengths_ref,
    block,
    rest_tiles,
    fall,
    sums,
    parts,
    packed,
    send_sem,
    recv_sem,
    pair_send,
    pair_recv,
    local_sem,
    part_send,
    part_recv,
    kv_send,
    kv_recv,
):
    z_lo = lax.axis_index("batch_0")
    core = lax.axis_index("batch_2")
    z_hi = lax.axis_index("seq_1")
    me = {"x": lax.axis_index("batch_1"), "y": lax.axis_index("seq_0"), "z": z_hi * 4 + z_lo}
    place = me["y"] * 2 + z_hi
    local_len = tokens_hbm.shape[0]
    span = HALO + local_len

    def toward(dim, way):
        spot = lax.rem(me[dim] + way + RING[dim], RING[dim])
        if dim == "x":
            return {"batch_1": spot}
        if dim == "y":
            return {"seq_0": spot}
        return {"batch_0": lax.rem(spot, 4), "seq_1": spot // 4}

    def beside(spot, c):
        return {"batch_2": c, "seq_0": spot // 2, "seq_1": lax.rem(spot, 2)}

    partner = {"batch_2": 1 - core}
    after = beside(lax.rem(place + 1, 8), core)

    barrier = pltpu.get_barrier_semaphore()
    friends = [toward(d, w) for d in "xz" for w in (1, -1)]
    for turn in range(8):
        for flip in range(2):
            if turn or flip:
                friends.append(beside(lax.rem(place + turn, 8), lax.rem(core + flip, 2)))
    for friend in friends:
        pl.semaphore_signal(barrier, inc=1, device_id=friend, device_id_type=MESH_ID)

    def remote(src, dst, sems, k, device):
        return pltpu.make_async_remote_copy(
            src_ref=src,
            dst_ref=dst,
            send_sem=sems[0].at[k],
            recv_sem=sems[1].at[k],
            device_id=device,
            device_id_type=MESH_ID,
        )

    mine = (me["z"], me["x"], pl.ds(2 * me["y"] + core, 1))
    own_heads = pl.ds(HEADS * core, HEADS)
    fetches = [
        pltpu.make_async_copy(src, dst, local_sem.at[k])
        for k, (src, dst) in enumerate(
            (
                (tokens_hbm, rows.at[0]),
                (attn_hbm, attn),
                (wkv_hbm, wkv),
                (wa_hbm.at[own_heads], gates.at[0]),
                (wi_hbm.at[own_heads], gates.at[1]),
            )
        )
    ]
    for fetch in fetches:
        fetch.start()

    shard = shard_ref[...].astype(jnp.float32)
    rest_tiles[...] = jnp.zeros_like(rest_tiles)
    for side in range(2):
        for unit in range(20):
            r, j = unit // 10, unit % 10
            column = COLS * side + 128 * j
            tile = 128 * (unit // 8)
            rest_tiles[side, unit % 8 : unit % 8 + 1, tile : tile + 128] = shard[
                8 + r : 9 + r, column : column + 128
            ]
        block[side, :, :COLS] = shard[:8, COLS * side : COLS * (side + 1)].astype(jnp.bfloat16)
        block[side, :, COLS:] = rest_tiles[side].astype(jnp.bfloat16)
    wide[mine] = block[pl.ds(core, 1)]
    lengths_ref[0] = jnp.full((8, 128), length_in[0], jnp.int32)
    spread = jnp.exp(-decay_ref[...])
    series = 1.0 / 5.0 - spread * (1.0 / 6.0)
    for c in (1.0 / 4.0, 1.0 / 3.0, 0.5, 1.0):
        series = c - spread * series
    fall[...] = (8.0 * spread) * series

    def place_rows(slot, start, raw):
        normed = normed_rows(raw, gain_ref[...])
        at = pl.ds(slot * span + start, raw.shape[0])
        for g in range(4):
            moved = f32_dot(normed[:, 640 * g : 640 * (g + 1)], order_ref[...])
            moved = moved.astype(jnp.bfloat16)
            ordered[at, pl.ds(256 * g, 256)] = moved[:, :256]
            ordered[at, pl.ds(1024 + 256 * g, 256)] = moved[:, 256:512]
            ordered[at, pl.ds(MAIN + 128 * g, 128)] = moved[:, 512:]

    def body_rows(slot, k):
        place_rows(slot, HALO + 256 * k, rows[slot, 256 * k : 256 * (k + 1), :])

    def edge_rows(slot):
        edge = halo[slot].astype(jnp.float32)
        blank = jnp.zeros((HALO - 4, edge.shape[1]), jnp.float32)
        place_rows(slot, 0, jnp.concatenate([blank, edge], axis=0))

    length = lengths_ref[0, 0:1, 0:1]

    def rotation(start):
        cosines, sines = [], []
        for lap in (start // 64, start // 64 + 1):
            at = pl.ds(place * (local_len // 64) + lap, 1)
            cosines.append(trig_ref[0, at, :] * trig_ref[2] - trig_ref[1, at, :] * trig_ref[3])
            sines.append(trig_ref[1, at, :] * trig_ref[2] + trig_ref[0, at, :] * trig_ref[3])
        return jnp.concatenate(cosines, axis=0), jnp.concatenate(sines, axis=0)

    def cache_rows(k):
        tops = []
        lane = lax.broadcasted_iota(jnp.int32, (128, 128), 1)
        for start in (128 * k, 256 + 128 * k):
            normed = normed_rows(attn[start : start + 128, :], attn_gain_ref[...])
            kv = f32_dot(normed, wkv[...])
            cosine, sine = rotation(start)
            turned = kv[:, :128] * cosine + pltpu.roll(kv[:, :128], 64, 1) * sine
            kv = jnp.concatenate([turned, kv[:, 128:]], axis=1).astype(jnp.bfloat16)
            at = place * local_len + start + lax.broadcasted_iota(jnp.int32, (128, 1), 0)
            inside = ((at >= length - W) & (at < length)).astype(jnp.float32)
            tops.append(kv.astype(jnp.float32) * inside)
        for t in range(4):
            upper = tops[0][:, 128 * t : 128 * (t + 1)]
            lower = tops[1][:, 128 * t : 128 * (t + 1)]
            even = jnp.where(lane < 64, upper, pltpu.roll(lower, 64, 1))
            odd = jnp.where(lane < 64, pltpu.roll(upper, 64, 1), lower)
            packed[2 * t, 128 * k : 128 * (k + 1), :] = even.astype(jnp.bfloat16)
            packed[2 * t + 1, 128 * k : 128 * (k + 1), :] = odd.astype(jnp.bfloat16)

    pl.semaphore_wait(barrier, len(friends))

    pair = (pair_send, pair_recv)
    given = remote(block.at[pl.ds(1 - core, 1)], wide.at[mine], pair, 0, partner)
    given.start()
    tail = remote(tail_rows, halo.at[0], pair, 1, after)
    length_copy = remote(lengths_ref.at[0], lengths_ref.at[1], pair, 2, partner)
    length_copy.start()
    rows_copy = remote(tokens_hbm, rows.at[1], pair, 3, partner)
    rows_copy.start()
    passed = remote(halo.at[0], halo.at[1], pair, 4, partner)

    def gather_copy(k):
        share, phase, way, step, half = COPIES[k]
        first, count, order = PLANS[share]
        dim = order[phase]
        spans = {d: pl.ds(0, RING[d]) for d in order[:phase]}
        spot = lax.rem(me[dim] - way * step + RING[dim], RING[dim])
        spans[dim] = pl.ds(spot, 1)
        for d in order[phase + 1 :]:
            spans[d] = pl.ds(me[d], 1)
        if "y" in order[:phase]:
            spans["y"] = pl.ds(4 * half, 4)
        else:
            y_at = spot if dim == "y" else me["y"]
            spans["y"] = pl.ds(2 * y_at + half, 1)
        piece = wide.at[
            spans["z"], spans["x"], spans["y"], pl.ds(0, 8), pl.ds(first * 128, count * 128)
        ]
        return remote(piece, piece, (send_sem, recv_sem), k, toward(dim, way))

    def start_own():
        fetches[0].wait()
        last = rows[0, local_len - 8 :, :].astype(jnp.float32)
        tail_rows[...] = last[4:].astype(jnp.bfloat16)
        body_rows(0, 0)
        tail.start()

    def start_other():
        rows_copy.wait()
        body_rows(1, 0)

    def pass_halo():
        tail.wait()
        passed.start()
        edge_rows(0)

    def start_cache():
        fetches[1].wait()
        fetches[2].wait()
        cache_rows(0)

    def end_halo():
        passed.wait()
        edge_rows(1)

    tasks = [
        (0.0, start_own),
        (10.0, lambda: body_rows(0, 1)),
        (14.0, pass_halo),
        (16.0, start_other),
        (19.0, lambda: body_rows(1, 1)),
        (22.0, start_cache),
        (25.0, lambda: cache_rows(1)),
        (28.0, end_halo),
    ]
    given.wait()
    started = {}
    for what, k, when in ORDER:
        if what == "send":
            started[k] = gather_copy(k)
            started[k].start()
        else:
            while tasks and tasks[0][0] <= when:
                tasks.pop(0)[1]()
            started[k].wait_recv()
    for _, task in tasks:
        task()

    def kv_copy(turn):
        spot = lax.rem(place + turn, 8)
        return pltpu.make_async_remote_copy(
            src_ref=packed.at[spot],
            dst_ref=cached.at[place],
            send_sem=kv_send.at[turn],
            recv_sem=kv_recv.at[turn],
            device_id=beside(spot, core),
            device_id_type=MESH_ID,
        )

    kv_copies = [kv_copy(turn) for turn in range(1, 8)]
    for copy in kv_copies:
        copy.start()
    local = pltpu.make_async_copy(packed.at[place], cached.at[place], local_sem.at[5])
    local.start()
    fetches[3].wait()
    fetches[4].wait()
    length_copy.wait()

    for z in range(8):
        rest = wide[z, :, :, :, COLS:].reshape(256, WIDE - COLS)
        sorted_rows = f32_dot(sort_ref[...], rest).astype(jnp.bfloat16)
        for r in range(2):
            for j in range(10):
                unit = r * 10 + j
                row = z % 4 * 128 + r * 64 + z // 4 * 32
                left[row : row + 32, 128 * j : 128 * (j + 1)] = sorted_rows[
                    32 * (unit % 8) : 32 * (unit % 8) + 32,
                    128 * (unit // 8) : 128 * (unit // 8 + 1),
                ]

    later_rows = (
        lax.broadcasted_iota(jnp.int32, (256, 256), 1)
        > lax.broadcasted_iota(jnp.int32, (256, 256), 0)
    ).astype(jnp.bfloat16)
    lengths = (length, lengths_ref[1, 0:1, 0:1])

    def of_head(head):
        return pl.ds(pl.multiple_of(head * HD, HD), HD)

    def project(head, proj):
        weight = wide[:, :, :, :, of_head(head)].reshape(MAIN, HD)
        total = f32_dot(ordered[:, :MAIN], weight)
        total = total + f32_dot(ordered[:, MAIN:], left[:, of_head(head)])
        proj[...] = total.astype(jnp.bfloat16).astype(jnp.float32)

    def fold(head, proj):
        columns = of_head(head)
        channels = pl.ds(pl.multiple_of((HEADS * core + head) * HD, HD), HD)
        taps = conv_ref[:, channels]
        pace = fall[:, channels]
        for slot in range(2):
            base = slot * span
            edge = proj[base : base + HALO, :]
            proj[base : base + HALO, :] = jnp.where(place > 0, edge, 0.0)
        for slot in range(2):
            base = slot * span
            log_total = jnp.zeros((1, HD), jnp.float32)
            state = jnp.zeros((1, HD), jnp.float32)
            for part in range(local_len // 256):
                first = base + HALO - 3 + 256 * part
                conv_sum = taps[0:1, :] * proj[pl.ds(first, 256), :]
                for offset in range(1, 4):
                    tap = taps[offset : offset + 1, :]
                    conv_sum = conv_sum + tap * proj[pl.ds(first + offset, 256), :]
                x_conv = conv_sum.astype(jnp.bfloat16)
                gate_a = f32_dot(x_conv, gates[0, head])
                gate_i = f32_dot(x_conv, gates[1, head])
                at = place * local_len + 256 * part
                at = at + lax.broadcasted_iota(jnp.int32, (256, 1), 0)
                valid = (at < lengths[slot]).astype(jnp.float32)
                drop = pace * sigmoid(gate_a)
                t = jnp.tanh(drop)
                twice = 2.0 * t
                push = twice * lax.rsqrt(jnp.maximum(twice * (1.0 + t), 1e-37))
                push = push * sigmoid(gate_i) * x_conv.astype(jnp.float32) * valid
                kept = -drop * valid
                high = kept.astype(jnp.bfloat16)
                low = (kept - high.astype(jnp.float32)).astype(jnp.bfloat16)
                later = f32_dot(later_rows, high) + f32_dot(later_rows, low)
                add = jnp.sum(jnp.exp(later) * push, axis=0, keepdims=True)
                log_part = jnp.sum(kept, axis=0, keepdims=True)
                state = jnp.exp(log_part) * state + add
                log_total = log_total + log_part
            spots = place * local_len + lax.broadcasted_iota(jnp.int32, (8, local_len), 1)
            wanted = lengths[slot] - 3 + lax.broadcasted_iota(jnp.int32, (8, local_len), 0)
            picker = (spots == wanted).astype(jnp.bfloat16)
            picked = f32_dot(picker, proj[base + HALO : base + span, :].astype(jnp.bfloat16))
            sums[slot, 0:1, columns] = log_total
            sums[slot, 1:2, columns] = state
            sums[slot, 2:5, columns] = picked[0:3]

    def head_pair(k, carry):
        project(2 * k + 1, proj_odd)
        fold(2 * k, proj_even)
        project(2 * k + 2, proj_even)
        fold(2 * k + 1, proj_odd)
        return carry

    sums[...] = jnp.zeros_like(sums)
    project(0, proj_even)
    lax.fori_loop(0, HEADS // 2, head_pair, 0)
    fold(HEADS - 1, proj_even)

    for slot in range(2):
        for k in range(4):
            whole = sums[slot]
            if k:
                whole = pltpu.roll(whole, COLS - 320 * k, 1)
            parts[slot, k] = whole[:, :384]

    def part_copy(slot, k):
        return pltpu.make_async_remote_copy(
            src_ref=parts.at[slot, k],
            dst_ref=arrived.at[place],
            send_sem=part_send.at[slot * 4 + k],
            recv_sem=part_recv.at[place],
            device_id=beside(4 * core + k, lax.rem(core + slot, 2)),
            device_id_type=MESH_ID,
        )

    def is_own(slot, k):
        return jnp.logical_and(slot == 0, place == 4 * core + k)

    for slot in range(2):
        for k in range(4):

            @pl.when(jnp.logical_not(is_own(slot, k)))
            def _(slot=slot, k=k):
                part_copy(slot, k).start()

    for k in range(4):

        @pl.when(is_own(0, k))
        def _(k=k):
            copy = pltpu.make_async_copy(parts.at[0, k], arrived.at[place], local_sem.at[6])
            copy.start()
            copy.wait()

    local.wait()
    for copy in kv_copies:
        copy.wait()
    near = core == place // 4
    for spot in range(8):

        @pl.when(jnp.logical_not(jnp.logical_and(near, place == spot)))
        def _(spot=spot):
            pltpu.make_async_remote_copy(
                src_ref=parts.at[0, 0],
                dst_ref=arrived.at[spot],
                send_sem=part_send.at[0],
                recv_sem=part_recv.at[spot],
                device_id=partner,
                device_id_type=MESH_ID,
            ).wait_recv()

    for slot in range(2):
        for k in range(4):

            @pl.when(jnp.logical_not(is_own(slot, k)))
            def _(slot=slot, k=k):
                part_copy(slot, k).wait_send()

    for k in sorted(started):
        started[k].wait_send()


def finish_kernel(arrived, cached, state_out, conv_out, cache_out):
    width = state_out.shape[1]
    state = jnp.zeros((1, width), jnp.float32)
    conv = jnp.zeros((3, width), jnp.float32)
    for spot in range(8):
        state = jnp.exp(arrived[spot, 0:1, :width]) * state + arrived[spot, 1:2, :width]
        conv = conv + arrived[spot, 2:5, :width]
    state_out[...] = state
    conv_out[...] = conv.astype(jnp.bfloat16)
    half = cached.shape[1]
    for k in range(4):
        both = cached[k].astype(jnp.float32) + cached[k + 4].astype(jnp.float32)
        turned = both.T.astype(jnp.bfloat16)
        cache_out[:, 2 * half * k : 2 * half * k + half] = turned[:64]
        cache_out[:, 2 * half * k + half : 2 * half * (k + 1)] = turned[64:]


def rotation_tables():
    spacing = 10000.0 ** (-np.arange(64) / 64)
    tables = []
    for step in (64, 1):
        angles = step * np.arange(64)[:, None] * spacing[None, :]
        tables.append(np.concatenate([np.cos(angles), np.cos(angles)], axis=1))
        tables.append(np.concatenate([-np.sin(angles), np.sin(angles)], axis=1))
    return jnp.asarray(np.stack(tables), jnp.float32)


def prefill(length, tokens, attn_in, w_kv, w_a, w_i, shard, gain, attn_gain, decay, conv_w):
    order, sort = column_orders()
    local_len, feature_dim = tokens.shape
    vmem = pl.BlockSpec(memory_space=pltpu.VMEM)
    hbm = pl.BlockSpec(memory_space=pl.ANY)
    dma = pltpu.SemaphoreType.DMA
    span = HALO + local_len
    arrived, cached = pl.pallas_call(
        prefill_kernel,
        out_shape=(
            jax.ShapeDtypeStruct((8, 8, 384), jnp.float32),
            jax.ShapeDtypeStruct((8, local_len // 2, 128), jnp.bfloat16),
        ),
        in_specs=[pl.BlockSpec(memory_space=pltpu.SMEM)] + [hbm] * 5 + [vmem] * 8,
        out_specs=(hbm, hbm),
        scratch_shapes=[
            pltpu.VMEM((8, 4, 8, 8, WIDE), jnp.bfloat16),
            pltpu.VMEM((2, local_len, feature_dim), jnp.bfloat16),
            pltpu.VMEM((2 * span, feature_dim), jnp.bfloat16),
            pltpu.VMEM((LEFT, COLS), jnp.bfloat16),
            pltpu.VMEM((2 * span, HD), jnp.float32),
            pltpu.VMEM((2 * span, HD), jnp.float32),
            pltpu.VMEM((local_len, feature_dim), jnp.bfloat16),
            pltpu.VMEM(w_kv.shape, jnp.bfloat16),
            pltpu.VMEM((2, HEADS, HD, HD), jnp.bfloat16),
            pltpu.VMEM((2, 4, feature_dim), jnp.bfloat16),
            pltpu.VMEM((4, feature_dim), jnp.bfloat16),
            pltpu.VMEM((2, 8, 128), jnp.int32),
            pltpu.VMEM((2, 8, WIDE), jnp.bfloat16),
            pltpu.VMEM((2, 8, WIDE - COLS), jnp.float32),
            pltpu.VMEM((1, feature_dim), jnp.float32),
            pltpu.VMEM((2, 8, COLS), jnp.float32),
            pltpu.VMEM((2, 4, 8, 384), jnp.float32),
            pltpu.VMEM((8, local_len // 2, 128), jnp.bfloat16),
            dma((len(COPIES),)),
            dma((len(COPIES),)),
            dma((5,)),
            dma((5,)),
            dma((7,)),
            dma((8,)),
            dma((8,)),
            dma((8,)),
            dma((8,)),
        ],
        compiler_params=pltpu.CompilerParams(
            collective_id=0, has_side_effects=True, vmem_limit_bytes=63 * 2**20
        ),
    )(
        length, tokens, attn_in, w_kv, w_a, w_i, shard, gain, attn_gain, decay, conv_w,
        order, sort, rotation_tables(),
    )
    return pl.pallas_call(
        finish_kernel,
        out_shape=(
            jax.ShapeDtypeStruct((1, feature_dim // 8), jnp.float32),
            jax.ShapeDtypeStruct((3, feature_dim // 8), jnp.bfloat16),
            jax.ShapeDtypeStruct((64, W), jnp.bfloat16),
        ),
        in_specs=[vmem, vmem],
        out_specs=(vmem, vmem, vmem),
    )(arrived, cached)


def on_device(
    tokens, attn_in, lengths, norm_gain, attn_gain, w_x, conv_w, w_a, w_i, lru_decay, w_kv
):
    lru_state, conv_state, cache_columns = prefill(
        lengths,
        tokens[0],
        attn_in[0],
        w_kv,
        w_a,
        w_i,
        w_x,
        norm_gain[None],
        attn_gain[None],
        lru_decay[None],
        conv_w,
    )
    return (lru_state, conv_state[None], cache_columns.T[None])


def solution(mesh):
    split = Mesh(mesh.devices.reshape(4, 4, 2, 4, 2), BATCH_SEQ)
    in_specs = (
        P(BATCH, SEQ, None),
        P(BATCH, SEQ, None),
        P(BATCH),
        P(),
        P(),
        P(BATCH_SEQ, None),
        P(),
        P(),
        P(),
        P(),
        P(),
    )
    out_specs = (P(BATCH, SEQ), P(BATCH, None, SEQ), P(BATCH, None, SEQ))
    return jax.shard_map(
        on_device, mesh=split, in_specs=in_specs, out_specs=out_specs, check_vma=False
    )
```

```python
import heapq

import jax
import jax.numpy as jnp
import numpy as np
from jax import lax
from jax.experimental import pallas as pl
from jax.experimental.pallas import tpu as pltpu
from jax.sharding import Mesh
from jax.sharding import PartitionSpec as P

HD = 256
W = 2048
SEQ = ("seq_0", "seq_1")
BATCH = ("batch_0", "batch_1", "batch_2")
BATCH_SEQ = BATCH + SEQ
MESH_ID = pl.DeviceIdType.MESH

RING = {"x": 4, "y": 4, "z": 8}
PLANS = (
    (0, 2, "zyx", None),
    (2, 2, "zxy", None),
    (4, 2, "zyx", None),
    (6, 2, "zxy", None),
    (8, 2, "xzy", (5, 0)),
    (10, 3, "yxz", None),
)
TASKS = (
    (0.0, 2.4),
    (9.8, 2.0),
    (12.1, 1.0),
    (14.4, 2.0),
    (16.7, 2.0),
    (19.0, 2.6),
    (21.3, 2.6),
    (23.5, 1.0),
)
HEADS = 5
COLS = HEADS * HD
WIDE = 13 * 128
MAIN = 2048
LEFT = 512
HALO = 16


def phase_copies(plans, share, phase):
    size = RING[plans[share][2][phase]]
    copies = []
    for step in range(size // 2):
        for half in (0, 1):
            for way in (1, -1):
                if step < size // 2 - 1 or half == (way < 0):
                    copies.append((share, phase, way, step, half))
    return copies


def gather_schedule(plans, task_times):
    count = len(plans)
    waiting, copies = {}, []
    for share in range(count):
        for phase in range(3):
            for c in phase_copies(plans, share, phase):
                _, _, way, step, half = c
                if step:
                    waiting[c] = {(share, phase, way, step - 1, half)}
                elif phase:
                    waiting[c] = set(phase_copies(plans, share, phase - 1))
                else:
                    gate = plans[share][3]
                    waiting[c] = set(phase_copies(plans, *gate)) if gate else set()
                copies.append(c)
    readers = {}
    for c in copies:
        for need in waiting[c]:
            readers.setdefault(need, []).append(c)
    index = {c: k for k, c in enumerate(copies)}
    missing = [sum(c[0] == s for c in copies) for s in range(count)]
    free, arrivals, order = {}, [], []
    now, stage = 0.0, 0
    tasks = list(enumerate(task_times))

    def send(c):
        share, phase, way, _, _ = c
        volume = plans[share][1]
        for dim in plans[share][2][:phase]:
            volume *= RING[dim]
        link = (plans[share][2][phase], way)
        free[link] = max(now, free.get(link, 0.0)) + volume * 2048 / 46.6e3
        heapq.heappush(arrivals, (free[link] + 1.8, index[c]))
        order.append(("send", index[c]))

    for half in (0, 1):
        for c in copies:
            if not waiting[c] and c[4] == half:
                send(c)
        order.append(("half", half))
    while arrivals or stage < count - 1:
        while arrivals and arrivals[0][0] <= now:
            c = copies[heapq.heappop(arrivals)[1]]
            order.append(("recv", index[c]))
            missing[c[0]] -= 1
            for d in readers.get(c, ()):
                waiting[d].discard(c)
                if not waiting[d]:
                    send(d)
        if tasks and tasks[0][1][0] <= now:
            number, (_, length) = tasks.pop(0)
            order.append(("task", number))
            now += length
        elif stage < count - 1 and not missing[stage] and not missing[-1] and not tasks:
            order.append(("stage", stage))
            now += 3.2 if stage else 2.6
            stage += 1
        else:
            pend = [arrivals[0][0]] if arrivals else []
            if tasks:
                pend.append(tasks[0][1][0])
            now = max(now, min(pend))
    return copies, order

COPIES, ORDER = gather_schedule(PLANS, TASKS)


def f32_dot(a, b):
    return jnp.dot(a, b, preferred_element_type=jnp.float32)


def normed_rows(raw, gain):
    wide = raw.astype(jnp.float32)
    inverse = lax.rsqrt(jnp.mean(wide * wide, axis=-1, keepdims=True) + 1e-06)
    return (wide * inverse * gain).astype(jnp.bfloat16)


def sigmoid(values):
    return 1.0 / (1.0 + jnp.exp(-values))


def prefill_kernel(
    length_in,
    tokens_hbm,
    attn_hbm,
    wkv_hbm,
    wa_hbm,
    wi_hbm,
    shard_ref,
    gain_ref,
    attn_gain_ref,
    decay_ref,
    conv_ref,
    trig_ref,
    arrived,
    cached,
    wide,
    rows,
    ordered,
    left,
    proj_even,
    proj_odd,
    attn,
    wkv,
    gates,
    halo,
    order_ref,
    sort_ref,
    tail_rows,
    lengths_ref,
    block,
    rest_tiles,
    fall,
    sums,
    parts,
    packed,
    send_sem,
    recv_sem,
    pair_send,
    pair_recv,
    local_sem,
    part_send,
    part_recv,
    kv_send,
    kv_recv,
):
    z_lo = lax.axis_index("batch_0")
    core = lax.axis_index("batch_2")
    z_hi = lax.axis_index("seq_1")
    me = {"x": lax.axis_index("batch_1"), "y": lax.axis_index("seq_0"), "z": z_hi * 4 + z_lo}
    place = me["y"] * 2 + z_hi
    local_len = tokens_hbm.shape[0]
    span = HALO + local_len

    def toward(dim, way):
        spot = lax.rem(me[dim] + way + RING[dim], RING[dim])
        if dim == "x":
            return {"batch_1": spot}
        if dim == "y":
            return {"seq_0": spot}
        return {"batch_0": lax.rem(spot, 4), "seq_1": spot // 4}

    def beside(spot, c):
        return {"batch_2": c, "seq_0": spot // 2, "seq_1": lax.rem(spot, 2)}

    partner = {"batch_2": 1 - core}
    after = beside(lax.rem(place + 1, 8), core)

    barrier = pltpu.get_barrier_semaphore()
    friends = [toward(d, w) for d in "xz" for w in (1, -1)]
    for turn in range(8):
        for flip in range(2):
            if turn or flip:
                friends.append(beside(lax.rem(place + turn, 8), lax.rem(core + flip, 2)))
    for friend in friends:
        pl.semaphore_signal(barrier, inc=1, device_id=friend, device_id_type=MESH_ID)

    def remote(src, dst, sems, k, device):
        return pltpu.make_async_remote_copy(
            src_ref=src,
            dst_ref=dst,
            send_sem=sems[0].at[k],
            recv_sem=sems[1].at[k],
            device_id=device,
            device_id_type=MESH_ID,
        )

    mine = (me["z"], me["x"], pl.ds(2 * me["y"] + core, 1))
    own_heads = pl.ds(HEADS * core, HEADS)
    fetches = [
        pltpu.make_async_copy(src, dst, local_sem.at[k])
        for k, (src, dst) in enumerate(
            (
                (tokens_hbm, rows.at[0]),
                (attn_hbm, attn),
                (wkv_hbm, wkv),
                (wa_hbm.at[own_heads], gates.at[0]),
                (wi_hbm.at[own_heads], gates.at[1]),
            )
        )
    ]
    for fetch in fetches:
        fetch.start()

    shard = shard_ref[...].astype(jnp.float32)
    rest_tiles[...] = jnp.zeros_like(rest_tiles)
    for side in range(2):
        for unit in range(20):
            r, j = unit // 10, unit % 10
            column = COLS * side + 128 * j
            tile = 128 * (unit // 8)
            rest_tiles[side, unit % 8 : unit % 8 + 1, tile : tile + 128] = shard[
                8 + r : 9 + r, column : column + 128
            ]
        block[side, :, :COLS] = shard[:8, COLS * side : COLS * (side + 1)].astype(jnp.bfloat16)
        block[side, :, COLS:] = rest_tiles[side].astype(jnp.bfloat16)
    wide[mine] = block[pl.ds(core, 1)]
    lengths_ref[0] = jnp.full((8, 128), length_in[0], jnp.int32)
    spread = jnp.exp(-decay_ref[...][None])
    series = 1.0 / 5.0 - spread * (1.0 / 6.0)
    for c in (1.0 / 4.0, 1.0 / 3.0, 0.5, 1.0):
        series = c - spread * series
    fall[...] = (8.0 * spread) * series

    feature = lax.broadcasted_iota(jnp.int32, (640, 1), 0)
    unit = (feature * 6554) >> 16
    i = feature - 10 * unit
    spot = (unit >> 4) * 8 + ((unit >> 1) & 3) * 2 + ((unit >> 3) & 1)
    target = jnp.where(
        i < 8,
        (unit & 1) * 256 + spot * 8 + i,
        512 + (i - 8) * 64 + (unit & 1) * 32 + spot,
    )
    lanes = lax.broadcasted_iota(jnp.int32, (640, 640), 1)
    order_ref[...] = (lanes == target).astype(jnp.float32).astype(jnp.bfloat16)
    row = lax.broadcasted_iota(jnp.int32, (256, 1), 0)
    lanes = lax.broadcasted_iota(jnp.int32, (256, 256), 1)
    source = (row & 31) * 8 + (row >> 5)
    sort_ref[...] = (lanes == source).astype(jnp.float32).astype(jnp.bfloat16)

    def place_rows(slot, start, raw):
        normed = normed_rows(raw, gain_ref[...][None])
        at = pl.ds(slot * span + start, raw.shape[0])
        for g in range(4):
            moved = f32_dot(normed[:, 640 * g : 640 * (g + 1)], order_ref[...])
            moved = moved.astype(jnp.bfloat16)
            ordered[at, pl.ds(256 * g, 256)] = moved[:, :256]
            ordered[at, pl.ds(1024 + 256 * g, 256)] = moved[:, 256:512]
            ordered[at, pl.ds(MAIN + 128 * g, 128)] = moved[:, 512:]

    def body_rows(slot, k):
        place_rows(slot, HALO + 256 * k, rows[slot, 256 * k : 256 * (k + 1), :])

    def edge_rows(slot):
        edge = halo[slot].astype(jnp.float32)
        blank = jnp.zeros((HALO - 4, edge.shape[1]), jnp.float32)
        place_rows(slot, 0, jnp.concatenate([blank, edge], axis=0))

    length = lengths_ref[0, 0:1, 0:1]

    def rotation(start):
        cosines, sines = [], []
        for lap in (start // 64, start // 64 + 1):
            at = pl.ds(place * (local_len // 64) + lap, 1)
            cosines.append(trig_ref[0, at, :] * trig_ref[2] - trig_ref[1, at, :] * trig_ref[3])
            sines.append(trig_ref[1, at, :] * trig_ref[2] + trig_ref[0, at, :] * trig_ref[3])
        return jnp.concatenate(cosines, axis=0), jnp.concatenate(sines, axis=0)

    def cache_rows(k):
        tops = []
        lane = lax.broadcasted_iota(jnp.int32, (128, 128), 1)
        for start in (128 * k, 256 + 128 * k):
            normed = normed_rows(attn[start : start + 128, :], attn_gain_ref[...][None])
            kv = f32_dot(normed, wkv[...])
            cosine, sine = rotation(start)
            turned = kv[:, :128] * cosine + pltpu.roll(kv[:, :128], 64, 1) * sine
            kv = jnp.concatenate([turned, kv[:, 128:]], axis=1).astype(jnp.bfloat16)
            at = place * local_len + start + lax.broadcasted_iota(jnp.int32, (128, 1), 0)
            inside = ((at >= length - W) & (at < length)).astype(jnp.float32)
            tops.append(kv.astype(jnp.float32) * inside)
        for t in range(4):
            upper = tops[0][:, 128 * t : 128 * (t + 1)]
            lower = tops[1][:, 128 * t : 128 * (t + 1)]
            even = jnp.where(lane < 64, upper, pltpu.roll(lower, 64, 1))
            odd = jnp.where(lane < 64, pltpu.roll(upper, 64, 1), lower)
            packed[2 * t, 128 * k : 128 * (k + 1), :] = even.astype(jnp.bfloat16)
            packed[2 * t + 1, 128 * k : 128 * (k + 1), :] = odd.astype(jnp.bfloat16)

    pl.semaphore_wait(barrier, len(friends))

    pair = (pair_send, pair_recv)
    given = remote(block.at[pl.ds(1 - core, 1)], wide.at[mine], pair, 0, partner)
    given.start()
    tail = remote(tail_rows, halo.at[0], pair, 1, after)
    length_copy = remote(lengths_ref.at[0], lengths_ref.at[1], pair, 2, partner)
    length_copy.start()
    rows_copy = remote(tokens_hbm, rows.at[1], pair, 3, partner)
    rows_copy.start()
    passed = remote(halo.at[0], halo.at[1], pair, 4, partner)

    def gather_copy(k):
        share, phase, way, step, half = COPIES[k]
        first, count, order, _ = PLANS[share]
        dim = order[phase]
        spans = {d: pl.ds(0, RING[d]) for d in order[:phase]}
        spot = lax.rem(me[dim] - way * step + RING[dim], RING[dim])
        spans[dim] = pl.ds(spot, 1)
        for d in order[phase + 1 :]:
            spans[d] = pl.ds(me[d], 1)
        if "y" in order[:phase]:
            spans["y"] = pl.ds(4 * half, 4)
        else:
            y_at = spot if dim == "y" else me["y"]
            spans["y"] = pl.ds(2 * y_at + lax.rem(core + half, 2), 1)
        piece = wide.at[
            spans["z"], spans["x"], spans["y"], pl.ds(0, 8), pl.ds(first * 128, count * 128)
        ]
        return remote(piece, piece, (send_sem, recv_sem), k, toward(dim, way))

    def start_own():
        fetches[0].wait()
        last = rows[0, local_len - 8 :, :].astype(jnp.float32)
        tail_rows[...] = last[4:].astype(jnp.bfloat16)
        body_rows(0, 0)
        tail.start()

    def start_other():
        rows_copy.wait()
        body_rows(1, 0)

    def pass_halo():
        tail.wait()
        passed.start()
        edge_rows(0)

    def start_cache():
        fetches[1].wait()
        fetches[2].wait()
        cache_rows(0)

    def end_halo():
        passed.wait()
        edge_rows(1)

    tasks = (
        start_own,
        lambda: body_rows(0, 1),
        pass_halo,
        start_other,
        lambda: body_rows(1, 1),
        start_cache,
        lambda: cache_rows(1),
        end_halo,
    )

    def kv_copy(turn):
        spot = lax.rem(place + turn, 8)
        return pltpu.make_async_remote_copy(
            src_ref=packed.at[spot],
            dst_ref=cached.at[place],
            send_sem=kv_send.at[turn],
            recv_sem=kv_recv.at[turn],
            device_id=beside(spot, core),
            device_id_type=MESH_ID,
        )

    kv_copies = [kv_copy(turn) for turn in range(1, 8)]
    local = pltpu.make_async_copy(packed.at[place], cached.at[place], local_sem.at[5])

    def sort_rest():
        for z in range(8):
            rest = wide[z, :, :, :, COLS:].reshape(256, WIDE - COLS)
            sorted_rows = f32_dot(sort_ref[...], rest).astype(jnp.bfloat16)
            for unit in range(20):
                r, j = unit // 10, unit % 10
                row = z % 4 * 128 + r * 64 + z // 4 * 32
                left[row : row + 32, 128 * j : 128 * (j + 1)] = sorted_rows[
                    32 * (unit % 8) : 32 * (unit % 8) + 32,
                    128 * (unit // 8) : 128 * (unit // 8 + 1),
                ]

    later_rows = (
        lax.broadcasted_iota(jnp.int32, (256, 256), 1)
        > lax.broadcasted_iota(jnp.int32, (256, 256), 0)
    ).astype(jnp.bfloat16)

    def of_head(head):
        return pl.ds(head * HD, HD)

    def project(head, proj):
        weight = wide[:, :, :, :, of_head(head)].reshape(MAIN, HD)
        total = f32_dot(ordered[:, :MAIN], weight)
        total = total + f32_dot(ordered[:, MAIN:], left[:, of_head(head)])
        proj[...] = total.astype(jnp.bfloat16).astype(jnp.float32)

    def fold(head, proj):
        lengths = (length, lengths_ref[1, 0:1, 0:1])
        columns = of_head(head)
        channels = pl.ds(pl.multiple_of((HEADS * core + head) * HD, HD), HD)
        taps = conv_ref[:, channels]
        pace = fall[:, channels]
        for slot in range(2):
            base = slot * span
            edge = proj[base : base + HALO, :]
            proj[base : base + HALO, :] = jnp.where(place > 0, edge, 0.0)
        for slot in range(2):
            base = slot * span
            log_total = jnp.zeros((1, HD), jnp.float32)
            state = jnp.zeros((1, HD), jnp.float32)
            for part in range(local_len // 256):
                first = base + HALO - 3 + 256 * part
                conv_sum = taps[0:1, :] * proj[pl.ds(first, 256), :]
                for offset in range(1, 4):
                    tap = taps[offset : offset + 1, :]
                    conv_sum = conv_sum + tap * proj[pl.ds(first + offset, 256), :]
                x_conv = conv_sum.astype(jnp.bfloat16)
                gate_a = f32_dot(x_conv, gates[0, head])
                gate_i = f32_dot(x_conv, gates[1, head])
                at = place * local_len + 256 * part
                at = at + lax.broadcasted_iota(jnp.int32, (256, 1), 0)
                valid = (at < lengths[slot]).astype(jnp.float32)
                drop = pace * sigmoid(gate_a)
                t = jnp.tanh(drop)
                twice = 2.0 * t
                push = twice * lax.rsqrt(jnp.maximum(twice * (1.0 + t), 1e-37))
                push = push * sigmoid(gate_i) * x_conv.astype(jnp.float32) * valid
                kept = -drop * valid
                high = kept.astype(jnp.bfloat16)
                low = (kept - high.astype(jnp.float32)).astype(jnp.bfloat16)
                later = f32_dot(later_rows, high) + f32_dot(later_rows, low)
                add = jnp.sum(jnp.exp(later) * push, axis=0, keepdims=True)
                log_part = jnp.sum(kept, axis=0, keepdims=True)
                state = jnp.exp(log_part) * state + add
                log_total = log_total + log_part
            spots = place * local_len + lax.broadcasted_iota(jnp.int32, (8, local_len), 1)
            wanted = lengths[slot] - 3 + lax.broadcasted_iota(jnp.int32, (8, local_len), 0)
            picker = (spots == wanted).astype(jnp.bfloat16)
            picked = f32_dot(picker, proj[base + HALO : base + span, :].astype(jnp.bfloat16))
            sums[slot, 0:1, columns] = log_total
            sums[slot, 1:2, columns] = state
            sums[slot, 2:5, columns] = picked[0:3]

    projs = (proj_even, proj_odd)

    def head_stage(head):
        if head == 0:
            fetches[3].wait()
            fetches[4].wait()
            length_copy.wait()
            sort_rest()
        project(head, projs[head % 2])
        if head:
            fold(head - 1, projs[(head - 1) % 2])

    sums[...] = jnp.zeros_like(sums)
    started = {}
    last_send = max(n for n, (what, _) in enumerate(ORDER) if what == "send")
    for n, (what, k) in enumerate(ORDER):
        if what == "send":
            started[k] = gather_copy(k)
            started[k].start()
        elif what == "recv":
            started[k].wait_recv()
        elif what == "task":
            tasks[k]()
        elif what == "stage":
            head_stage(k)
        elif k == 0:
            given.wait()
        if n == last_send:
            local.start()
            for copy in kv_copies:
                copy.start()
    fold(HEADS - 1, projs[(HEADS - 1) % 2])

    for slot in range(2):
        for k in range(4):
            whole = sums[slot]
            if k:
                whole = pltpu.roll(whole, COLS - 320 * k, 1)
            parts[slot, k] = whole[:, :384]

    def part_copy(slot, k):
        return pltpu.make_async_remote_copy(
            src_ref=parts.at[slot, k],
            dst_ref=arrived.at[place],
            send_sem=part_send.at[slot * 4 + k],
            recv_sem=part_recv.at[place],
            device_id=beside(4 * core + k, lax.rem(core + slot, 2)),
            device_id_type=MESH_ID,
        )

    def is_own(slot, k):
        return jnp.logical_and(slot == 0, place == 4 * core + k)

    for slot in range(2):
        for k in range(4):

            @pl.when(jnp.logical_not(is_own(slot, k)))
            def _(slot=slot, k=k):
                part_copy(slot, k).start()

    for k in range(4):

        @pl.when(is_own(0, k))
        def _(k=k):
            copy = pltpu.make_async_copy(parts.at[0, k], arrived.at[place], local_sem.at[6])
            copy.start()
            copy.wait()

    local.wait()
    for copy in kv_copies:
        copy.wait()
    near = core == place // 4
    for spot in range(8):

        @pl.when(jnp.logical_not(jnp.logical_and(near, place == spot)))
        def _(spot=spot):
            pltpu.make_async_remote_copy(
                src_ref=parts.at[0, 0],
                dst_ref=arrived.at[spot],
                send_sem=part_send.at[0],
                recv_sem=part_recv.at[spot],
                device_id=partner,
                device_id_type=MESH_ID,
            ).wait_recv()

    for slot in range(2):
        for k in range(4):

            @pl.when(jnp.logical_not(is_own(slot, k)))
            def _(slot=slot, k=k):
                part_copy(slot, k).wait_send()

    for k in sorted(started):
        started[k].wait_send()


def finish_kernel(arrived, cached, state_out, conv_out, cache_out):
    width = state_out.shape[1]
    state = jnp.zeros((1, width), jnp.float32)
    conv = jnp.zeros((3, width), jnp.float32)
    for spot in range(8):
        state = jnp.exp(arrived[spot, 0:1, :width]) * state + arrived[spot, 1:2, :width]
        conv = conv + arrived[spot, 2:5, :width]
    state_out[...] = state
    conv_out[...] = conv.astype(jnp.bfloat16)
    half = cached.shape[1]
    for k in range(4):
        both = cached[k].astype(jnp.float32) + cached[k + 4].astype(jnp.float32)
        turned = both.T.astype(jnp.bfloat16)
        cache_out[:, 2 * half * k : 2 * half * k + half] = turned[:64]
        cache_out[:, 2 * half * k + half : 2 * half * (k + 1)] = turned[64:]


def rotation_tables():
    spacing = 10000.0 ** (-np.arange(64) / 64)
    tables = []
    for step in (64, 1):
        angles = step * np.arange(64)[:, None] * spacing[None, :]
        tables.append(np.concatenate([np.cos(angles), np.cos(angles)], axis=1))
        tables.append(np.concatenate([-np.sin(angles), np.sin(angles)], axis=1))
    return jnp.asarray(np.stack(tables), jnp.float32)


def prefill(length, tokens, attn_in, w_kv, w_a, w_i, shard, gain, attn_gain, decay, conv_w):
    local_len, feature_dim = tokens.shape
    vmem = pl.BlockSpec(memory_space=pltpu.VMEM)
    hbm = pl.BlockSpec(memory_space=pl.ANY)
    dma = pltpu.SemaphoreType.DMA
    span = HALO + local_len
    arrived, cached = pl.pallas_call(
        prefill_kernel,
        out_shape=(
            jax.ShapeDtypeStruct((8, 8, 384), jnp.float32),
            jax.ShapeDtypeStruct((8, local_len // 2, 128), jnp.bfloat16),
        ),
        in_specs=[pl.BlockSpec(memory_space=pltpu.SMEM)] + [hbm] * 5 + [vmem] * 6,
        out_specs=(hbm, hbm),
        scratch_shapes=[
            pltpu.VMEM((8, 4, 8, 8, WIDE), jnp.bfloat16),
            pltpu.VMEM((2, local_len, feature_dim), jnp.bfloat16),
            pltpu.VMEM((2 * span, feature_dim), jnp.bfloat16),
            pltpu.VMEM((LEFT, COLS), jnp.bfloat16),
            pltpu.VMEM((2 * span, HD), jnp.float32),
            pltpu.VMEM((2 * span, HD), jnp.float32),
            pltpu.VMEM((local_len, feature_dim), jnp.bfloat16),
            pltpu.VMEM(w_kv.shape, jnp.bfloat16),
            pltpu.VMEM((2, HEADS, HD, HD), jnp.bfloat16),
            pltpu.VMEM((2, 4, feature_dim), jnp.bfloat16),
            pltpu.VMEM((640, 640), jnp.bfloat16),
            pltpu.VMEM((256, 256), jnp.bfloat16),
            pltpu.VMEM((4, feature_dim), jnp.bfloat16),
            pltpu.VMEM((2, 8, 128), jnp.int32),
            pltpu.VMEM((2, 8, WIDE), jnp.bfloat16),
            pltpu.VMEM((2, 8, WIDE - COLS), jnp.float32),
            pltpu.VMEM((1, feature_dim), jnp.float32),
            pltpu.VMEM((2, 8, COLS), jnp.float32),
            pltpu.VMEM((2, 4, 8, 384), jnp.float32),
            pltpu.VMEM((8, local_len // 2, 128), jnp.bfloat16),
            dma((len(COPIES),)),
            dma((len(COPIES),)),
            dma((5,)),
            dma((5,)),
            dma((7,)),
            dma((8,)),
            dma((8,)),
            dma((8,)),
            dma((8,)),
        ],
        compiler_params=pltpu.CompilerParams(
            collective_id=0, has_side_effects=True, vmem_limit_bytes=63 * 2**20
        ),
    )(
        length, tokens, attn_in, w_kv, w_a, w_i, shard, gain, attn_gain, decay, conv_w,
        rotation_tables(),
    )
    return pl.pallas_call(
        finish_kernel,
        out_shape=(
            jax.ShapeDtypeStruct((1, feature_dim // 8), jnp.float32),
            jax.ShapeDtypeStruct((3, feature_dim // 8), jnp.bfloat16),
            jax.ShapeDtypeStruct((64, W), jnp.bfloat16),
        ),
        in_specs=[vmem, vmem],
        out_specs=(vmem, vmem, vmem),
    )(arrived, cached)


def on_device(
    tokens, attn_in, lengths, norm_gain, attn_gain, w_x, conv_w, w_a, w_i, lru_decay, w_kv
):
    lru_state, conv_state, cache_columns = prefill(
        lengths,
        tokens[0],
        attn_in[0],
        w_kv,
        w_a,
        w_i,
        w_x,
        norm_gain,
        attn_gain,
        lru_decay,
        conv_w,
    )
    return (lru_state, conv_state[None], cache_columns.T[None])


def solution(mesh):
    split = Mesh(mesh.devices.reshape(4, 4, 2, 4, 2), BATCH_SEQ)
    in_specs = (
        P(BATCH, SEQ, None),
        P(BATCH, SEQ, None),
        P(BATCH),
        P(),
        P(),
        P(BATCH_SEQ, None),
        P(),
        P(),
        P(),
        P(),
        P(),
    )
    out_specs = (P(BATCH, SEQ), P(BATCH, None, SEQ), P(BATCH, None, SEQ))
    return jax.shard_map(
        on_device, mesh=split, in_specs=in_specs, out_specs=out_specs, check_vma=False
    )
```

```python
import heapq

import jax
import jax.numpy as jnp
import numpy as np
from jax import lax
from jax.experimental import pallas as pl
from jax.experimental.pallas import tpu as pltpu
from jax.sharding import Mesh
from jax.sharding import PartitionSpec as P

HD = 256
W = 2048
SEQ = ("seq_0", "seq_1")
BATCH = ("batch_0", "batch_1", "batch_2")
BATCH_SEQ = BATCH + SEQ
MESH_ID = pl.DeviceIdType.MESH

RING = {"x": 4, "y": 4, "z": 8}
PLANS = (
    (0, 2, "zxy", None),
    (2, 2, "zyx", None),
    (4, 2, "yzx", None),
    (6, 2, "zxy", None),
    (8, 2, "zxy", (1, 0)),
    (10, 3, "xyz", None),
)
TASKS = (
    (0.0, 2.8),
    (11.0, 1.6),
    (13.7, 0.7),
    (16.4, 1.6),
    (19.0, 1.6),
    (21.7, 2.2),
    (24.4, 2.0),
    (27.1, 0.7),
)
HEADS = 5
COLS = HEADS * HD
WIDE = 13 * 128
MAIN = 2048
LEFT = 512
HALO = 16


def phase_copies(plans, share, phase):
    size = RING[plans[share][2][phase]]
    copies = []
    for step in range(size // 2):
        for half in (0, 1):
            for way in (1, -1):
                if step < size // 2 - 1 or half == (way < 0):
                    copies.append((share, phase, way, step, half))
    return copies


def gather_schedule(plans, task_times):
    count = len(plans)
    waiting, copies = {}, []
    for share in range(count):
        for phase in range(3):
            for c in phase_copies(plans, share, phase):
                _, _, way, step, half = c
                if phase and step:
                    waiting[c] = {(share, phase, way, step - 1, half)}
                elif phase:
                    waiting[c] = set(phase_copies(plans, share, phase - 1))
                else:
                    gate = plans[share][3]
                    waiting[c] = set(phase_copies(plans, *gate)) if gate else set()
                copies.append(c)
    readers = {}
    for c in copies:
        for need in waiting[c]:
            readers.setdefault(need, []).append(c)
    index = {c: k for k, c in enumerate(copies)}
    missing = [sum(c[0] == s for c in copies) for s in range(count)]
    free, arrivals, order = {}, [], []
    now, stage = 0.0, 0
    tasks = list(enumerate(task_times))

    def send(c):
        share, phase, way, step, _ = c
        hops = 1 if phase else step + 1
        volume = plans[share][1] * hops
        for dim in plans[share][2][:phase]:
            volume *= RING[dim]
        link = (plans[share][2][phase], way)
        free[link] = max(now, free.get(link, 0.0)) + volume * 2048 / 46.6e3
        heapq.heappush(arrivals, (free[link] + 1.6 + 0.7 * hops, index[c]))
        order.append(("send", index[c]))

    for half in (0, 1):
        for c in copies:
            if not waiting[c] and c[4] == half:
                send(c)
        order.append(("half", half))
    while arrivals or stage < count - 1:
        while arrivals and arrivals[0][0] <= now:
            c = copies[heapq.heappop(arrivals)[1]]
            order.append(("recv", index[c]))
            missing[c[0]] -= 1
            for d in readers.get(c, ()):
                waiting[d].discard(c)
                if not waiting[d]:
                    send(d)
        if tasks and tasks[0][1][0] <= now:
            number, (_, length) = tasks.pop(0)
            order.append(("task", number))
            now += length
        elif stage < count - 1 and not missing[stage] and not missing[-1] and not tasks:
            order.append(("stage", stage))
            now += 3.0 if stage else 2.6
            stage += 1
        else:
            pend = [arrivals[0][0]] if arrivals else []
            if tasks:
                pend.append(tasks[0][1][0])
            now = max(now, min(pend))
    return copies, order
COPIES, ORDER = gather_schedule(PLANS, TASKS)


def f32_dot(a, b):
    return jnp.dot(a, b, preferred_element_type=jnp.float32)


def normed_rows(raw, gain):
    wide = raw.astype(jnp.float32)
    inverse = lax.rsqrt(jnp.mean(wide * wide, axis=-1, keepdims=True) + 1e-06)
    return (wide * inverse * gain).astype(jnp.bfloat16)


def sigmoid(values):
    return 1.0 / (1.0 + jnp.exp(-values))


def prefill_kernel(
    length_in,
    tokens_hbm,
    attn_hbm,
    wkv_hbm,
    wa_hbm,
    wi_hbm,
    shard_ref,
    gain_ref,
    attn_gain_ref,
    decay_ref,
    conv_ref,
    trig_ref,
    arrived,
    cached,
    wide,
    rows,
    ordered,
    left,
    proj_even,
    proj_odd,
    attn,
    wkv,
    gates,
    halo,
    order_ref,
    sort_ref,
    tail_rows,
    lengths_ref,
    block,
    rest_tiles,
    fall,
    sums,
    parts,
    packed,
    send_sem,
    recv_sem,
    pair_send,
    pair_recv,
    local_sem,
    part_send,
    part_recv,
    kv_send,
    kv_recv,
):
    z_lo = lax.axis_index("batch_0")
    core = lax.axis_index("batch_2")
    z_hi = lax.axis_index("seq_1")
    me = {"x": lax.axis_index("batch_1"), "y": lax.axis_index("seq_0"), "z": z_hi * 4 + z_lo}
    place = me["y"] * 2 + z_hi
    local_len = tokens_hbm.shape[0]
    span = HALO + local_len

    def toward(dim, way):
        spot = lax.rem(me[dim] + way + RING[dim], RING[dim])
        if dim == "x":
            return {"batch_1": spot}
        if dim == "y":
            return {"seq_0": spot}
        return {"batch_0": lax.rem(spot, 4), "seq_1": spot // 4}

    def beside(spot, c):
        return {"batch_2": c, "seq_0": spot // 2, "seq_1": lax.rem(spot, 2)}

    partner = {"batch_2": 1 - core}
    after = beside(lax.rem(place + 1, 8), core)

    barrier = pltpu.get_barrier_semaphore()
    friends = [toward("x", away) for away in (1, 2, 3)]
    friends += [toward("z", away) for away in (1, 2, 3, -1, -2, -3)]
    for turn in range(8):
        for flip in range(2):
            if turn or flip:
                friends.append(beside(lax.rem(place + turn, 8), lax.rem(core + flip, 2)))
    for friend in friends:
        pl.semaphore_signal(barrier, inc=1, device_id=friend, device_id_type=MESH_ID)

    def remote(src, dst, sems, k, device):
        return pltpu.make_async_remote_copy(
            src_ref=src,
            dst_ref=dst,
            send_sem=sems[0].at[k],
            recv_sem=sems[1].at[k],
            device_id=device,
            device_id_type=MESH_ID,
        )

    mine = (me["z"], me["x"], pl.ds(2 * me["y"] + core, 1))
    own_heads = pl.ds(HEADS * core, HEADS)
    fetches = [
        pltpu.make_async_copy(src, dst, local_sem.at[k])
        for k, (src, dst) in enumerate(
            (
                (tokens_hbm, rows.at[0]),
                (attn_hbm, attn),
                (wkv_hbm, wkv),
                (wa_hbm.at[own_heads], gates.at[0]),
                (wi_hbm.at[own_heads], gates.at[1]),
            )
        )
    ]
    for fetch in fetches:
        fetch.start()

    shard = shard_ref[...].astype(jnp.float32)
    rest_tiles[...] = jnp.zeros_like(rest_tiles)
    for side in range(2):
        for unit in range(20):
            r, j = unit // 10, unit % 10
            column = COLS * side + 128 * j
            tile = 128 * (unit // 8)
            rest_tiles[side, unit % 8 : unit % 8 + 1, tile : tile + 128] = shard[
                8 + r : 9 + r, column : column + 128
            ]
        block[side, :, :COLS] = shard[:8, COLS * side : COLS * (side + 1)].astype(jnp.bfloat16)
        block[side, :, COLS:] = rest_tiles[side].astype(jnp.bfloat16)
    wide[mine] = block[pl.ds(core, 1)]
    lengths_ref[0] = jnp.full((8, 128), length_in[0], jnp.int32)
    def place_rows(slot, start, raw):
        normed = normed_rows(raw, gain_ref[...][None])
        at = pl.ds(slot * span + start, raw.shape[0])
        for g in range(4):
            moved = f32_dot(normed[:, 640 * g : 640 * (g + 1)], order_ref[...])
            moved = moved.astype(jnp.bfloat16)
            ordered[at, pl.ds(256 * g, 256)] = moved[:, :256]
            ordered[at, pl.ds(1024 + 256 * g, 256)] = moved[:, 256:512]
            ordered[at, pl.ds(MAIN + 128 * g, 128)] = moved[:, 512:]

    def body_rows(slot, k):
        place_rows(slot, HALO + 256 * k, rows[slot, 256 * k : 256 * (k + 1), :])

    def edge_rows(slot):
        edge = halo[slot].astype(jnp.float32)
        blank = jnp.zeros((HALO - 4, edge.shape[1]), jnp.float32)
        place_rows(slot, 0, jnp.concatenate([blank, edge], axis=0))

    length = lengths_ref[0, 0:1, 0:1]

    def rotation(start):
        cosines, sines = [], []
        for lap in (start // 64, start // 64 + 1):
            at = pl.ds(place * (local_len // 64) + lap, 1)
            cosines.append(trig_ref[0, at, :] * trig_ref[2] - trig_ref[1, at, :] * trig_ref[3])
            sines.append(trig_ref[1, at, :] * trig_ref[2] + trig_ref[0, at, :] * trig_ref[3])
        return jnp.concatenate(cosines, axis=0), jnp.concatenate(sines, axis=0)

    def cache_rows(k):
        tops = []
        lane = lax.broadcasted_iota(jnp.int32, (128, 128), 1)
        for start in (128 * k, 256 + 128 * k):
            normed = normed_rows(attn[start : start + 128, :], attn_gain_ref[...][None])
            kv = f32_dot(normed, wkv[...])
            cosine, sine = rotation(start)
            turned = kv[:, :128] * cosine + pltpu.roll(kv[:, :128], 64, 1) * sine
            kv = jnp.concatenate([turned, kv[:, 128:]], axis=1).astype(jnp.bfloat16)
            at = place * local_len + start + lax.broadcasted_iota(jnp.int32, (128, 1), 0)
            inside = ((at >= length - W) & (at < length)).astype(jnp.float32)
            tops.append(kv.astype(jnp.float32) * inside)
        for t in range(4):
            upper = tops[0][:, 128 * t : 128 * (t + 1)]
            lower = tops[1][:, 128 * t : 128 * (t + 1)]
            even = jnp.where(lane < 64, upper, pltpu.roll(lower, 64, 1))
            odd = jnp.where(lane < 64, pltpu.roll(upper, 64, 1), lower)
            packed[2 * t, 128 * k : 128 * (k + 1), :] = even.astype(jnp.bfloat16)
            packed[2 * t + 1, 128 * k : 128 * (k + 1), :] = odd.astype(jnp.bfloat16)

    pl.semaphore_wait(barrier, len(friends))

    pair = (pair_send, pair_recv)
    given = remote(block.at[pl.ds(1 - core, 1)], wide.at[mine], pair, 0, partner)
    given.start()
    tail = remote(tail_rows, halo.at[0], pair, 1, after)
    length_copy = remote(lengths_ref.at[0], lengths_ref.at[1], pair, 2, partner)
    length_copy.start()
    rows_copy = remote(tokens_hbm, rows.at[1], pair, 3, partner)
    rows_copy.start()
    passed = remote(halo.at[0], halo.at[1], pair, 4, partner)

    def gather_copy(k):
        share, phase, way, step, half = COPIES[k]
        first, count, order, _ = PLANS[share]
        dim = order[phase]
        spans = {d: pl.ds(0, RING[d]) for d in order[:phase]}
        away = way if phase else way * (step + 1)
        back = way * step if phase else 0
        spot = lax.rem(me[dim] - back + RING[dim], RING[dim])
        spans[dim] = pl.ds(spot, 1)
        for d in order[phase + 1 :]:
            spans[d] = pl.ds(me[d], 1)
        if "y" in order[:phase]:
            spans["y"] = pl.ds(4 * half, 4)
        else:
            y_at = spot if dim == "y" else me["y"]
            spans["y"] = pl.ds(2 * y_at + lax.rem(core + half, 2), 1)
        piece = wide.at[
            spans["z"], spans["x"], spans["y"], pl.ds(0, 8), pl.ds(first * 128, count * 128)
        ]
        return remote(piece, piece, (send_sem, recv_sem), k, toward(dim, away))

    def start_own():
        spread = jnp.exp(-decay_ref[...][None])
        series = 1.0 / 5.0 - spread * (1.0 / 6.0)
        for c in (1.0 / 4.0, 1.0 / 3.0, 0.5, 1.0):
            series = c - spread * series
        fall[...] = (8.0 * spread) * series

        feature = lax.broadcasted_iota(jnp.int32, (640, 1), 0)
        unit = (feature * 6554) >> 16
        i = feature - 10 * unit
        spot = (unit >> 4) * 8 + ((unit >> 1) & 3) * 2 + ((unit >> 3) & 1)
        target = jnp.where(
            i < 8,
            (unit & 1) * 256 + spot * 8 + i,
            512 + (i - 8) * 64 + (unit & 1) * 32 + spot,
        )
        lanes = lax.broadcasted_iota(jnp.int32, (640, 640), 1)
        order_ref[...] = (lanes == target).astype(jnp.float32).astype(jnp.bfloat16)
        row = lax.broadcasted_iota(jnp.int32, (256, 1), 0)
        lanes = lax.broadcasted_iota(jnp.int32, (256, 256), 1)
        source = (row & 31) * 8 + (row >> 5)
        sort_ref[...] = (lanes == source).astype(jnp.float32).astype(jnp.bfloat16)
        fetches[0].wait()
        last = rows[0, local_len - 8 :, :].astype(jnp.float32)
        tail_rows[...] = last[4:].astype(jnp.bfloat16)
        body_rows(0, 0)
        tail.start()

    def start_other():
        rows_copy.wait()
        body_rows(1, 0)

    def pass_halo():
        tail.wait()
        passed.start()
        edge_rows(0)

    def start_cache():
        fetches[1].wait()
        fetches[2].wait()
        cache_rows(0)

    def end_halo():
        passed.wait()
        edge_rows(1)

    tasks = (
        start_own,
        lambda: body_rows(0, 1),
        pass_halo,
        start_other,
        lambda: body_rows(1, 1),
        start_cache,
        lambda: cache_rows(1),
        end_halo,
    )

    def kv_copy(turn):
        spot = lax.rem(place + turn, 8)
        return pltpu.make_async_remote_copy(
            src_ref=packed.at[spot],
            dst_ref=cached.at[place],
            send_sem=kv_send.at[turn],
            recv_sem=kv_recv.at[turn],
            device_id=beside(spot, core),
            device_id_type=MESH_ID,
        )

    kv_copies = [kv_copy(turn) for turn in range(1, 8)]
    local = pltpu.make_async_copy(packed.at[place], cached.at[place], local_sem.at[5])

    def sort_rest():
        for z in range(8):
            rest = wide[z, :, :, :, COLS:].reshape(256, WIDE - COLS)
            sorted_rows = f32_dot(sort_ref[...], rest).astype(jnp.bfloat16)
            for unit in range(20):
                r, j = unit // 10, unit % 10
                row = z % 4 * 128 + r * 64 + z // 4 * 32
                left[row : row + 32, 128 * j : 128 * (j + 1)] = sorted_rows[
                    32 * (unit % 8) : 32 * (unit % 8) + 32,
                    128 * (unit // 8) : 128 * (unit // 8 + 1),
                ]

    later_rows = (
        lax.broadcasted_iota(jnp.int32, (256, 256), 1)
        > lax.broadcasted_iota(jnp.int32, (256, 256), 0)
    ).astype(jnp.bfloat16)

    def of_head(head):
        return pl.ds(head * HD, HD)

    def project(head, proj):
        weight = wide[:, :, :, :, of_head(head)].reshape(MAIN, HD)
        total = f32_dot(ordered[:, :MAIN], weight)
        total = total + f32_dot(ordered[:, MAIN:], left[:, of_head(head)])
        proj[...] = total.astype(jnp.bfloat16).astype(jnp.float32)

    def fold(head, proj):
        lengths = (length, lengths_ref[1, 0:1, 0:1])
        columns = of_head(head)
        channels = pl.ds(pl.multiple_of((HEADS * core + head) * HD, HD), HD)
        taps = conv_ref[:, channels]
        pace = fall[:, channels]
        for slot in range(2):
            base = slot * span
            edge = proj[base : base + HALO, :]
            proj[base : base + HALO, :] = jnp.where(place > 0, edge, 0.0)
        for slot in range(2):
            base = slot * span
            log_total = jnp.zeros((1, HD), jnp.float32)
            state = jnp.zeros((1, HD), jnp.float32)
            for part in range(local_len // 256):
                first = base + HALO - 3 + 256 * part
                conv_sum = taps[0:1, :] * proj[pl.ds(first, 256), :]
                for offset in range(1, 4):
                    tap = taps[offset : offset + 1, :]
                    conv_sum = conv_sum + tap * proj[pl.ds(first + offset, 256), :]
                x_conv = conv_sum.astype(jnp.bfloat16)
                gate_a = f32_dot(x_conv, gates[0, head])
                gate_i = f32_dot(x_conv, gates[1, head])
                at = place * local_len + 256 * part
                at = at + lax.broadcasted_iota(jnp.int32, (256, 1), 0)
                valid = (at < lengths[slot]).astype(jnp.float32)
                drop = pace * sigmoid(gate_a)
                t = jnp.tanh(drop)
                twice = 2.0 * t
                push = twice * lax.rsqrt(jnp.maximum(twice * (1.0 + t), 1e-37))
                push = push * sigmoid(gate_i) * x_conv.astype(jnp.float32) * valid
                kept = -drop * valid
                high = kept.astype(jnp.bfloat16)
                low = (kept - high.astype(jnp.float32)).astype(jnp.bfloat16)
                later = f32_dot(later_rows, high) + f32_dot(later_rows, low)
                add = jnp.sum(jnp.exp(later) * push, axis=0, keepdims=True)
                log_part = jnp.sum(kept, axis=0, keepdims=True)
                state = jnp.exp(log_part) * state + add
                log_total = log_total + log_part
            spots = place * local_len + lax.broadcasted_iota(jnp.int32, (8, local_len), 1)
            wanted = lengths[slot] - 3 + lax.broadcasted_iota(jnp.int32, (8, local_len), 0)
            picker = (spots == wanted).astype(jnp.bfloat16)
            picked = f32_dot(picker, proj[base + HALO : base + span, :].astype(jnp.bfloat16))
            sums[slot, 0:1, columns] = log_total
            sums[slot, 1:2, columns] = state
            sums[slot, 2:5, columns] = picked[0:3]

    projs = (proj_even, proj_odd)

    def head_stage(head):
        if head == 0:
            fetches[3].wait()
            fetches[4].wait()
            length_copy.wait()
            sort_rest()
        project(head, projs[head % 2])
        if head:
            fold(head - 1, projs[(head - 1) % 2])

    sums[...] = jnp.zeros_like(sums)
    started = {}
    last_send = max(n for n, (what, _) in enumerate(ORDER) if what == "send")
    for n, (what, k) in enumerate(ORDER):
        if what == "send":
            started[k] = gather_copy(k)
            started[k].start()
        elif what == "recv":
            started[k].wait_recv()
        elif what == "task":
            tasks[k]()
        elif what == "stage":
            head_stage(k)
        elif k == 0:
            given.wait()
        if n == last_send:
            local.start()
            for copy in kv_copies:
                copy.start()
    fold(HEADS - 1, projs[(HEADS - 1) % 2])

    for slot in range(2):
        for k in range(4):
            whole = sums[slot]
            if k:
                whole = pltpu.roll(whole, COLS - 320 * k, 1)
            parts[slot, k] = whole[:, :384]

    def part_copy(slot, k):
        return pltpu.make_async_remote_copy(
            src_ref=parts.at[slot, k],
            dst_ref=arrived.at[place],
            send_sem=part_send.at[slot * 4 + k],
            recv_sem=part_recv.at[place],
            device_id=beside(4 * core + k, lax.rem(core + slot, 2)),
            device_id_type=MESH_ID,
        )

    def is_own(slot, k):
        return jnp.logical_and(slot == 0, place == 4 * core + k)

    for slot in range(2):
        for k in range(4):

            @pl.when(jnp.logical_not(is_own(slot, k)))
            def _(slot=slot, k=k):
                part_copy(slot, k).start()

    for k in range(4):

        @pl.when(is_own(0, k))
        def _(k=k):
            copy = pltpu.make_async_copy(parts.at[0, k], arrived.at[place], local_sem.at[6])
            copy.start()
            copy.wait()

    local.wait()
    for copy in kv_copies:
        copy.wait()
    near = core == place // 4
    for spot in range(8):

        @pl.when(jnp.logical_not(jnp.logical_and(near, place == spot)))
        def _(spot=spot):
            pltpu.make_async_remote_copy(
                src_ref=parts.at[0, 0],
                dst_ref=arrived.at[spot],
                send_sem=part_send.at[0],
                recv_sem=part_recv.at[spot],
                device_id=partner,
                device_id_type=MESH_ID,
            ).wait_recv()

    for slot in range(2):
        for k in range(4):

            @pl.when(jnp.logical_not(is_own(slot, k)))
            def _(slot=slot, k=k):
                part_copy(slot, k).wait_send()

    for k in sorted(started):
        started[k].wait_send()


def finish_kernel(arrived, cached, state_out, conv_out, cache_out):
    width = state_out.shape[1]
    state = jnp.zeros((1, width), jnp.float32)
    conv = jnp.zeros((3, width), jnp.float32)
    for spot in range(8):
        state = jnp.exp(arrived[spot, 0:1, :width]) * state + arrived[spot, 1:2, :width]
        conv = conv + arrived[spot, 2:5, :width]
    state_out[...] = state
    conv_out[...] = conv.astype(jnp.bfloat16)
    half = cached.shape[1]
    for k in range(4):
        both = cached[k].astype(jnp.float32) + cached[k + 4].astype(jnp.float32)
        turned = both.T.astype(jnp.bfloat16)
        cache_out[:, 2 * half * k : 2 * half * k + half] = turned[:64]
        cache_out[:, 2 * half * k + half : 2 * half * (k + 1)] = turned[64:]


def rotation_tables():
    spacing = 10000.0 ** (-np.arange(64) / 64)
    tables = []
    for step in (64, 1):
        angles = step * np.arange(64)[:, None] * spacing[None, :]
        tables.append(np.concatenate([np.cos(angles), np.cos(angles)], axis=1))
        tables.append(np.concatenate([-np.sin(angles), np.sin(angles)], axis=1))
    return jnp.asarray(np.stack(tables), jnp.float32)


def prefill(length, tokens, attn_in, w_kv, w_a, w_i, shard, gain, attn_gain, decay, conv_w):
    local_len, feature_dim = tokens.shape
    vmem = pl.BlockSpec(memory_space=pltpu.VMEM)
    hbm = pl.BlockSpec(memory_space=pl.ANY)
    dma = pltpu.SemaphoreType.DMA
    span = HALO + local_len
    arrived, cached = pl.pallas_call(
        prefill_kernel,
        out_shape=(
            jax.ShapeDtypeStruct((8, 8, 384), jnp.float32),
            jax.ShapeDtypeStruct((8, local_len // 2, 128), jnp.bfloat16),
        ),
        in_specs=[pl.BlockSpec(memory_space=pltpu.SMEM)] + [hbm] * 5 + [vmem] * 6,
        out_specs=(hbm, hbm),
        scratch_shapes=[
            pltpu.VMEM((8, 4, 8, 8, WIDE), jnp.bfloat16),
            pltpu.VMEM((2, local_len, feature_dim), jnp.bfloat16),
            pltpu.VMEM((2 * span, feature_dim), jnp.bfloat16),
            pltpu.VMEM((LEFT, COLS), jnp.bfloat16),
            pltpu.VMEM((2 * span, HD), jnp.float32),
            pltpu.VMEM((2 * span, HD), jnp.float32),
            pltpu.VMEM((local_len, feature_dim), jnp.bfloat16),
            pltpu.VMEM(w_kv.shape, jnp.bfloat16),
            pltpu.VMEM((2, HEADS, HD, HD), jnp.bfloat16),
            pltpu.VMEM((2, 4, feature_dim), jnp.bfloat16),
            pltpu.VMEM((640, 640), jnp.bfloat16),
            pltpu.VMEM((256, 256), jnp.bfloat16),
            pltpu.VMEM((4, feature_dim), jnp.bfloat16),
            pltpu.VMEM((2, 8, 128), jnp.int32),
            pltpu.VMEM((2, 8, WIDE), jnp.bfloat16),
            pltpu.VMEM((2, 8, WIDE - COLS), jnp.float32),
            pltpu.VMEM((1, feature_dim), jnp.float32),
            pltpu.VMEM((2, 8, COLS), jnp.float32),
            pltpu.VMEM((2, 4, 8, 384), jnp.float32),
            pltpu.VMEM((8, local_len // 2, 128), jnp.bfloat16),
            dma((len(COPIES),)),
            dma((len(COPIES),)),
            dma((5,)),
            dma((5,)),
            dma((7,)),
            dma((8,)),
            dma((8,)),
            dma((8,)),
            dma((8,)),
        ],
        compiler_params=pltpu.CompilerParams(
            collective_id=0, has_side_effects=True, vmem_limit_bytes=63 * 2**20
        ),
    )(
        length, tokens, attn_in, w_kv, w_a, w_i, shard, gain, attn_gain, decay, conv_w,
        rotation_tables(),
    )
    return pl.pallas_call(
        finish_kernel,
        out_shape=(
            jax.ShapeDtypeStruct((1, feature_dim // 8), jnp.float32),
            jax.ShapeDtypeStruct((3, feature_dim // 8), jnp.bfloat16),
            jax.ShapeDtypeStruct((64, W), jnp.bfloat16),
        ),
        in_specs=[vmem, vmem],
        out_specs=(vmem, vmem, vmem),
    )(arrived, cached)


def on_device(
    tokens, attn_in, lengths, norm_gain, attn_gain, w_x, conv_w, w_a, w_i, lru_decay, w_kv
):
    lru_state, conv_state, cache_columns = prefill(
        lengths,
        tokens[0],
        attn_in[0],
        w_kv,
        w_a,
        w_i,
        w_x,
        norm_gain,
        attn_gain,
        lru_decay,
        conv_w,
    )
    return (lru_state, conv_state[None], cache_columns.T[None])


def solution(mesh):
    split = Mesh(mesh.devices.reshape(4, 4, 2, 4, 2), BATCH_SEQ)
    in_specs = (
        P(BATCH, SEQ, None),
        P(BATCH, SEQ, None),
        P(BATCH),
        P(),
        P(),
        P(BATCH_SEQ, None),
        P(),
        P(),
        P(),
        P(),
        P(),
    )
    out_specs = (P(BATCH, SEQ), P(BATCH, None, SEQ), P(BATCH, None, SEQ))
    return jax.shard_map(
        on_device, mesh=split, in_specs=in_specs, out_specs=out_specs, check_vma=False
    )
```
